256 devices in a mesh: patch: 32 (over y, x, core), rhs: 8 (over z).
Axes of the slice: x: 4, y: 4, z: 8, core: 2. Of those that a mesh axis runs over, the one named last changes fastest.
Arguments:
- rhs_vectors: float32 [256, 16, 384], P('patch', 'rhs'), may hold values from -8 to 8
- near_blocks: bfloat16 [256, 4, 384, 384], P('patch'), may hold values from -1 to 5, as said below
- neighbours: int32 [256, 4], P('patch'), may hold values from 0 to 255, as said below
- up_maps: float32 [256, 64, 384], P('patch'), may hold values from -0.3125 to 0.3125
- shift_up: float32 [256, 64, 64], P('patch'), may hold values from -0.25 to 0.25
- far_lists: int32 [32, 4], P('patch'), may hold values from 0 to 31, as said below
- translations: float32 [32, 4, 64, 64], P('patch'), may hold values from -0.375 to 0.375
- shift_down: float32 [256, 64, 64], P('patch'), may hold values from -0.75 to 0.75
- down_maps: float32 [256, 384, 64], P('patch'), may hold values from -0.375 to 0.375
Outputs:
- solution: float32 [256, 16, 384], P('patch', 'rhs')
- residual: float32 [256, 16, 384], P('patch', 'rhs')
The draws below stay inside these ranges and needn't reach their ends.
Inputs may be any that keep to these rules, and one draw needn't show every extreme that they name: `neighbours`: entry 0 of each row is the patch itself; every other entry names a patch of the same cell or of the cell just before or just after it, cyclically. `far_lists`: entry 0 of each row names the cell just before or just after the row's own cell, cyclically, and for cell 0 the cell just before it; every other entry names a cell other than the row's own. `near_blocks`: the blocks keep the operator's symmetric part positive definite.
All inputs are finite; a program needn't handle non-finite values.
Results may differ from the reference program's by a relative error of at most 0.008.
The reference program's roundings to bfloat16 on the way (of `rounded`) count: a program that leaves them out, or rounds other values in their place, can miss the bound.
Values may be sent and summed in bfloat16 or wider, within the bound.
A program may use at most 64 MiB of HBM per device.

```python
import math
import jax
import jax.numpy as jnp
from jax import lax

K = 16
W = 384
E = 64
NB = 4
FL = 4
ITERS = 2
PD = 8
PATCHES = 256
CELLS = 32


def draw_near_blocks(key, part):
    spread = 0.35 / math.sqrt(W * NB)
    noise = jax.random.normal(key, (PATCHES, NB, W, W), jnp.float32) * spread
    selfpart = (jnp.arange(NB) == 0).astype(jnp.float32)[:, None, None] * jnp.eye(W, dtype=jnp.float32) * 4.0
    return (noise + selfpart[None]).astype(jnp.bfloat16)


def draw_neighbours(key, part):
    labels = jnp.arange(PATCHES, dtype=jnp.int32)
    owner = labels // PD
    offset = jax.random.randint(jax.random.fold_in(key, 11), (PATCHES, NB), 0, 3 * PD, dtype=jnp.int32) - PD
    chosen = jnp.mod(owner[:, None] * PD + offset, PATCHES).astype(jnp.int32)
    return chosen.at[:, 0].set(labels)


def draw_far_lists(key, part):
    labels = jnp.arange(CELLS, dtype=jnp.int32)
    offset = jax.random.randint(jax.random.fold_in(key, 23), (CELLS, FL), 1, CELLS, dtype=jnp.int32)
    side = jax.random.randint(jax.random.fold_in(key, 29), (CELLS,), 0, 2, dtype=jnp.int32) * 2 - 1
    side = jnp.where(labels == 0, -1, side).astype(jnp.int32)
    offset = offset.at[:, 0].set(side)
    return jnp.mod(labels[:, None] + offset, CELLS).astype(jnp.int32)


def level_of(key, dims, cuts, low, high):
    gain, own = 1.0, jax.random.fold_in(key, 6)
    for position, shards_of in cuts:
        steps = jnp.exp(jax.random.uniform(jax.random.fold_in(own, position), (shards_of,), jnp.float32, low / len(cuts), high / len(cuts)))
        gain = gain * jnp.repeat(steps, dims[position] // shards_of).reshape([-1 if axis == position else 1 for axis in range(len(dims))])
    return gain


def normal_values(rng, extent, deviation, bound, split=(), kind=jnp.bfloat16):
    loudness = level_of(rng, extent, split, -0.22, 0.18) if split else 1.0
    drawn = jax.random.normal(rng, extent, jnp.float32) * deviation * loudness
    return jnp.minimum(jnp.maximum(drawn, -bound), bound).astype(kind)


def setup_inputs(seed: int = 0) -> dict:
    seeds = jax.random.split(jax.random.key(seed), 10)
    return {
        "rhs_vectors": normal_values(seeds[0], (PATCHES, K, W), 2.0, 8.0, ((0, 32), (1, 8)), jnp.float32),
        "near_blocks": draw_near_blocks(jax.random.fold_in(seeds[9], 71), 0),
        "neighbours": draw_neighbours(jax.random.fold_in(seeds[9], 71), 0),
        "up_maps": normal_values(seeds[3], (PATCHES, E, W), W ** -0.5, 0.3125, ((0, 32),), jnp.float32),
        "shift_up": normal_values(seeds[4], (PATCHES, E, E), (E * PD) ** -0.5, 0.25, ((0, 32),), jnp.float32),
        "far_lists": draw_far_lists(jax.random.fold_in(seeds[9], 71), 0),
        "translations": normal_values(seeds[6], (CELLS, FL, E, E), (E * FL) ** -0.5, 0.375, ((0, 32),), jnp.float32),
        "shift_down": normal_values(seeds[7], (PATCHES, E, E), E ** -0.5, 0.75, ((0, 32),), jnp.float32),
        "down_maps": normal_values(seeds[8], (PATCHES, W, E), (4 * E) ** -0.5, 0.375, ((0, 32),), jnp.float32),
    }


HIGH = lax.Precision.HIGHEST

def spd_solve(matrix, right):
    factor = jnp.linalg.cholesky(matrix)
    return jax.scipy.linalg.cho_solve((factor, True), right)

def gram(left, right):
    return jnp.einsum('pkw,plw->kl', left, right, precision=HIGH)

def mix(field, coeffs):
    return jnp.einsum('pkw,kl->plw', field, coeffs, precision=HIGH)

def operator(field, near_blocks, neighbours, up_maps, shift_up, far_lists, translations, shift_down, down_maps):
    rounded = lax.optimization_barrier(field.astype(jnp.bfloat16)).astype(jnp.float32)
    picked = rounded[neighbours]
    near = jnp.einsum('pjvw,pjkw->pkv', near_blocks.astype(jnp.float32), picked, precision=HIGH)
    moments = jnp.einsum('pew,pkw->pke', up_maps, field, precision=HIGH)
    cells = moments.reshape(CELLS, PD, K, E)
    shifts = shift_up.reshape(CELLS, PD, E, E)
    cell_moment = jnp.einsum('cpfe,cpke->ckf', shifts, cells, precision=HIGH)
    sources = cell_moment[far_lists]
    local_exp = jnp.einsum('cjfe,cjke->ckf', translations, sources, precision=HIGH)
    spread = jnp.repeat(local_exp, PD, axis=0)
    patch_exp = jnp.einsum('pfe,pke->pkf', shift_down, spread, precision=HIGH)
    far = jnp.einsum('pvf,pkf->pkv', down_maps, patch_exp, precision=HIGH)
    return near + far

def reference(rhs_vectors, near_blocks, neighbours, up_maps, shift_up, far_lists, translations, shift_down, down_maps):
    residual = rhs_vectors
    solution = jnp.zeros_like(residual)
    direction = residual
    current = gram(residual, residual)
    for step in range(ITERS):
        image = operator(direction, near_blocks, neighbours, up_maps, shift_up, far_lists, translations, shift_down, down_maps)
        curve = gram(direction, image)
        curve = 0.5 * (curve + curve.T)
        alpha = spd_solve(curve, current)
        solution = solution + mix(direction, alpha)
        residual = residual - mix(image, alpha)
        if step + 1 < ITERS:
            following = gram(residual, residual)
            beta = spd_solve(current, following)
            direction = residual + mix(direction, beta)
            current = following
    return (solution, residual)
```

```python
import jax
import jax.numpy as jnp
from jax import lax
from jax.experimental import pallas as pl
from jax.experimental.pallas import tpu as pltpu
from jax.sharding import PartitionSpec as P

F32 = jnp.float32
BF16 = jnp.bfloat16
HIGH = lax.Precision.HIGHEST
MESH = pl.DeviceIdType.MESH
PD, K, W, E, NB, FL = 8, 16, 384, 64, 4, 4
NT = (((1,), (1,)), ((), ()))
NN = (((1,), (0,)), ((), ()))


def dot(a, b, dims=NT, precision=None):
    return lax.dot_general(a, b, dims, precision=precision, preferred_element_type=F32)


def split(x):
    hi = x.astype(BF16)
    return hi, (x - hi.astype(F32)).astype(BF16)


def folded(x):
    return x + pltpu.roll(x, 64, 1)


def lane_of(shape):
    return lax.broadcasted_iota(jnp.int32, shape, 1)


def eliminate(top, *others):
    a = jnp.concatenate((top, *others), axis=0)
    lanes = lane_of(a.shape)
    for k in range(K):
        column = a[:, k : k + 1]
        row = a[k : k + 1, :]
        inverse = 1.0 / a[k : k + 1, k : k + 1]
        a = jnp.where(lanes == k, column * inverse, a - column * (row * inverse))
    return [a[K * (i + 1) : K * (i + 2), :] for i in range(len(others))]


def packed_grams(stack):
    full = dot(stack, stack)
    full = jnp.concatenate((full, jnp.zeros((4 * K, 128 - 4 * K), F32)), axis=1)

    def half(top, low):
        t = top + low
        t = t + pltpu.roll(t, 128 - K, 1)
        even = (lane_of((8, 128)) // K) % 2 == 0
        return jnp.where(even, t[:8], pltpu.roll(t[8:], K, 1))

    a = half(full[:K], full[K : 2 * K])
    b = half(full[2 * K : 3 * K], full[3 * K :])
    return jnp.where(lane_of((8, 128)) < 4 * K, a, pltpu.roll(b, 4 * K, 1))


def unpacked_grams(total):
    t = jnp.concatenate((total, pltpu.roll(total, 128 - K, 1)), axis=0)
    return t[:, :K], t[:, 2 * K : 3 * K], t[:, 4 * K : 5 * K], t[:, 6 * K : 7 * K]


def kernel(
    rhs_h, near_h, nbr_h, up_h, su_h, fl_h, tr_h, sd_h, dn_h,
    sol_o, res_o,
    rhs_v, near_v, nbr_s, up_v, su_v, fl_s, tr_v, sd_v, dn_v,
    g, hl, hr, s, sw, s2, xb, cst, tst, dst, mg, lg, lf, pg, wg, pc, cf,
    local_sem, near_sem,
    z_send, z_recv, f_send, hl_recv, hr_recv,
    m_send, m_recv, l_send, l_recv, p_send, p_recv, w_send, w_recv,
    c_send, c_recv, o_send, ol_recv, or_recv,
):
    me = lax.axis_index("patch")
    z = lax.axis_index("rhs")
    np_, nz = lax.axis_size("patch"), lax.axis_size("rhs")
    left, right = lax.rem(me + np_ - 1, np_), lax.rem(me + 1, np_)

    def load(i, src, dst):
        copy = pltpu.make_async_copy(src, dst, local_sem.at[i])
        copy.start()
        return copy

    c_rhs = load(0, rhs_h, rhs_v)
    c_up = load(1, up_h, up_v)
    c_su = load(2, su_h, su_v)
    c_nbr = load(3, nbr_h, nbr_s)
    c_fl = load(4, fl_h, fl_s)
    c_tr = load(5, tr_h, tr_v)
    c_sd = load(6, sd_h, sd_v)
    c_dn = load(7, dn_h, dn_v)
    c_near = []
    for p in range(PD):
        copy = pltpu.make_async_copy(near_h.at[p], near_v.at[p], near_sem.at[p])
        copy.start()
        c_near.append(copy)

    barrier = pltpu.get_barrier_semaphore()
    for d in range(1, np_):
        pl.semaphore_signal(barrier, inc=1, device_id=(lax.rem(me + d, np_), z), device_id_type=MESH)
    for d in range(1, nz):
        pl.semaphore_signal(barrier, inc=1, device_id=(me, lax.rem(z + d, nz)), device_id_type=MESH)

    pending = []

    def send(src, dst, ssem, rsem, device):
        copy = pltpu.make_async_remote_copy(
            src_ref=src, dst_ref=dst, send_sem=ssem, recv_sem=rsem, device_id=device, device_id_type=MESH
        )
        copy.start()
        pending.append(copy)

    def arrived(dst, ssem, rsem):
        pltpu.make_async_remote_copy(
            src_ref=dst, dst_ref=dst, send_sem=ssem, recv_sem=rsem, device_id=(right, z), device_id_type=MESH
        ).wait_recv()

    def spread_patch(buf, ssem, rsem):
        for d in range(1, np_):
            to = lax.rem(me + d, np_)
            send(buf.at[me], buf.at[me], ssem.at[d], rsem.at[me], (to, z))

    def gathered_patch(buf, ssem, rsem):
        for d in range(1, np_):
            frm = lax.rem(me + d, np_)
            arrived(buf.at[frm], ssem.at[d], rsem.at[frm])

    c_rhs.wait()
    own_hi, own_lo = [], []
    for p in range(PD):
        hi, lo = split(rhs_v[p])
        g[z, p, 0] = hi
        g[z, p, 1] = lo
        own_hi.append(hi)
        own_lo.append(lo)
    own_hi = jnp.concatenate(own_hi, axis=1)
    own_lo = jnp.concatenate(own_lo, axis=1)

    pl.semaphore_wait(barrier, np_ + nz - 2)

    z_order = (4, 3, 5, 2, 6, 1, 7)
    for d in z_order:
        send(g.at[z], g.at[z], z_send.at[d], z_recv.at[z], (me, lax.rem(z + d, nz)))

    def forward(zz, i):
        send(g.at[zz], hl.at[zz], f_send.at[2 * i], hl_recv.at[zz], (right, z))
        send(g.at[zz], hr.at[zz], f_send.at[2 * i + 1], hr_recv.at[zz], (left, z))

    forward(z, 0)

    c_up.wait()
    c_su.wait()
    for p in range(PD):
        hi, lo = split(dot(su_v[p], up_v[p], NN, HIGH))
        cst[:E, p * W : (p + 1) * W] = hi
        cst[E:, p * W : (p + 1) * W] = lo
    mine = folded(dot(own_hi, cst[...]) + dot(own_lo, cst[...]))
    mg[me] = mine
    spread_patch(mg, m_send, m_recv)

    c_tr.wait()
    for i in range(2):
        a, b = tr_v[0, 2 * i], tr_v[0, 2 * i + 1]
        hi, lo = split(jnp.concatenate((a, b), axis=1))
        tst[:E, i * 128 : (i + 1) * 128] = hi
        tst[E:, i * 128 : (i + 1) * 128] = lo

    c_sd.wait()
    c_dn.wait()
    for p in range(PD):
        hi, lo = split(dot(sd_v[p].T, dn_v[p], NN, HIGH))
        dst[p, :E] = hi
        dst[p, E:] = lo

    for i, d in enumerate((1, 7, 2, 6, 3, 5, 4)):
        zz = lax.rem(z + d, nz)
        arrived(g.at[zz], z_send.at[d], z_recv.at[zz])
        forward(zz, i + 1)

    def assembled(buf, base):
        for zz in range(8):
            for h in range(2):
                for p in range(PD):
                    s[base + p, h, 2 * zz : 2 * zz + 2, :] = buf[zz, p, h]

    assembled(g, PD)

    c_fl.wait()
    gathered_patch(mg, m_send, m_recv)
    src = [fl_s[0, j] for j in range(FL)]
    low2 = lane_of((2, 128)) < E
    chosen = jnp.concatenate(
        (jnp.where(low2, mg[src[0]], mg[src[1]]), jnp.where(low2, mg[src[2]], mg[src[3]])), axis=1
    )
    hi, lo = split(chosen)
    lg[z] = folded(dot(hi, tst[...]) + dot(lo, tst[...]))
    for d in z_order:
        send(lg.at[z], lg.at[z], l_send.at[d], l_recv.at[z], (me, lax.rem(z + d, nz)))

    for d in range(nz):
        zz = lax.rem(z + d, nz)
        arrived(hl.at[zz], f_send.at[0], hl_recv.at[zz])
        arrived(hr.at[zz], f_send.at[0], hr_recv.at[zz])
    assembled(hl, 0)
    assembled(hr, 2 * PD)

    c_nbr.wait()
    first = me * PD - PD
    total_patches = np_ * PD
    ids = [
        [
            jnp.minimum(lax.rem(nbr_s[j, p] - first + 2 * total_patches, total_patches), 3 * PD - 1)
            for j in range(NB)
        ]
        for p in range(PD)
    ]

    for d in range(1, nz):
        zz = lax.rem(z + d, nz)
        arrived(lg.at[zz], l_send.at[d], l_recv.at[zz])
    for zz in range(8):
        lf[2 * zz : 2 * zz + 2, :] = lg[zz]
    local0 = lf[...]

    def image_of(p, pick, lcat):
        blocks = jnp.concatenate([near_v[p, j] for j in range(NB)], axis=1)
        fields = jnp.concatenate([pick(ids[p][j]) for j in range(NB)], axis=1)
        far = dot(lcat, dst[p], NN)
        return dot(blocks, fields).T + (far[:K] + far[K:])

    lcat = jnp.concatenate(split(local0), axis=0)
    for p in range(PD):
        c_near[p].wait()
        hi, lo = split(image_of(p, lambda i: s[i, 0], lcat))
        sw[PD + p, 0] = hi
        sw[PD + p, 1] = lo

    def lanes_joined(ref, base):
        rows = ref.shape[1] * K
        return jnp.concatenate([ref[base + p].reshape(rows, W) for p in range(PD)], axis=1)

    joined_w = lanes_joined(sw, PD)
    pg[me] = packed_grams(jnp.concatenate((lanes_joined(s, PD), joined_w), axis=0))
    spread_patch(pg, p_send, p_recv)
    up_w = dot(joined_w, cst[...])
    up_w = folded(up_w[:K] + up_w[K:])
    low8 = lane_of((8, 128)) < E
    wg[me] = jnp.where(low8, up_w[:8], up_w[8:])
    spread_patch(wg, w_send, w_recv)
    send(sw.at[PD : 2 * PD], sw.at[0:PD], o_send.at[0], ol_recv, (right, z))
    send(sw.at[PD : 2 * PD], sw.at[2 * PD : 3 * PD], o_send.at[1], or_recv, (left, z))

    gathered_patch(pg, p_send, p_recv)
    rr, gg, gt, qq = unpacked_grams(jnp.sum(pg[...], axis=0))
    eye = (lax.broadcasted_iota(jnp.int32, (K, K), 0) == lane_of((K, K))).astype(F32)
    (a1,) = eliminate(0.5 * (gg + gt), rr)
    gtk, inv = eliminate(rr, gt, eye)
    aq = dot(a1, qq, NN, HIGH) - gg
    ka = dot(inv, a1, NN, HIGH)
    ag = dot(a1, gtk, NN, HIGH)
    beta_t = eye - ag + dot(aq, ka, NT, HIGH)
    rr1 = rr - dot(a1, gt, NN, HIGH) + dot(aq, a1, NT, HIGH)

    gathered_patch(wg, w_send, w_recv)
    us = [wg[src[j]] for j in range(FL)]
    rs = [pltpu.roll(u, E, 1) for u in us]
    chosen = jnp.concatenate(
        (
            jnp.concatenate((jnp.where(low8, us[0], rs[1]), jnp.where(low8, rs[0], us[1])), axis=0),
            jnp.concatenate((jnp.where(low8, us[2], rs[3]), jnp.where(low8, rs[2], us[3])), axis=0),
        ),
        axis=1,
    )
    hi, lo = split(chosen)
    local_w = folded(dot(hi, tst[...]) + dot(lo, tst[...]))
    local2 = dot(eye + beta_t, local0, NN, HIGH) - dot(a1, local_w, NN, HIGH)
    lcat = jnp.concatenate(split(local2), axis=0)

    first_co, second_co = eye + beta_t, -a1
    mixer = jnp.concatenate((first_co, first_co, second_co, second_co), axis=1)
    mhi = mixer.astype(BF16).astype(F32)
    mixer = jnp.concatenate((mhi, mixer - mhi), axis=0).astype(BF16)

    arrived(sw.at[0:PD], o_send.at[0], ol_recv)
    arrived(sw.at[2 * PD : 3 * PD], o_send.at[0], or_recv)
    def four(i):
        return jnp.concatenate((s[i].reshape(2 * K, W), sw[i].reshape(2 * K, W)), axis=0)

    for i in range(3 * PD):
        t = dot(mixer, four(i), NN)
        hi, lo = split(t[:K] + t[K:])
        xb[i] = hi
        if PD <= i < 2 * PD:
            s2[i - PD, 0] = hi
            s2[i - PD, 1] = lo

    for p in range(PD):
        hi, lo = split(image_of(p, lambda i: xb[i], lcat))
        s2[p, 2] = hi
        s2[p, 3] = lo

    pc[me] = packed_grams(lanes_joined(s2, 0))
    spread_patch(pc, c_send, c_recv)
    gathered_patch(pc, c_send, c_recv)
    _, gg, gt, _ = unpacked_grams(jnp.sum(pc[...], axis=0))
    (a2,) = eliminate(0.5 * (gg + gt), rr1)
    none = jnp.zeros((K, K), F32)
    cf[:K] = jnp.concatenate((a1, a1, none, none, a2, a2, none, none), axis=1)
    cf[K:] = jnp.concatenate((eye, eye, -a1, -a1, none, none, -a2, -a2), axis=1)
    coeffs = jnp.concatenate((cf[pl.ds(2 * z, 2), :], cf[pl.ds(K + 2 * z, 2), :]), axis=0)
    chi = coeffs.astype(BF16).astype(F32)
    coeffs = jnp.concatenate((chi, coeffs - chi), axis=0).astype(BF16)
    for p in range(PD):
        t = dot(coeffs, jnp.concatenate((four(PD + p), s2[p].reshape(4 * K, W)), axis=0), NN)
        t = t[:4] + t[4:]
        sol_o[p] = t[:2]
        res_o[p] = t[2:]

    for copy in pending:
        copy.wait_send()


def on_device(*args):
    args = list(args)
    args[2] = args[2].T
    args[8] = jnp.swapaxes(args[8], 1, 2)
    np_, nz = lax.axis_size("patch"), lax.axis_size("rhs")
    vm = pltpu.VMEM
    sem = pltpu.SemaphoreType.DMA
    scratch = [
        vm((PD, 2, W), F32),
        vm((PD, NB, W, W), BF16),
        pltpu.SMEM((NB, PD), jnp.int32),
        vm((PD, E, W), F32),
        vm((PD, E, E), F32),
        pltpu.SMEM((1, FL), jnp.int32),
        vm((1, FL, E, E), F32),
        vm((PD, E, E), F32),
        vm((PD, E, W), F32),
        vm((nz, PD, 2, 2, W), BF16),
        vm((nz, PD, 2, 2, W), BF16),
        vm((nz, PD, 2, 2, W), BF16),
        vm((3 * PD, 2, K, W), BF16),
        vm((3 * PD, 2, K, W), BF16),
        vm((PD, 4, K, W), BF16),
        vm((3 * PD, K, W), BF16),
        vm((2 * E, PD * W), BF16),
        vm((2 * E, FL * E), BF16),
        vm((PD, 2 * E, W), BF16),
        vm((np_, 2, 128), F32),
        vm((nz, 2, 128), F32),
        vm((K, 128), F32),
        vm((np_, 8, 128), F32),
        vm((np_, 8, 128), F32),
        vm((np_, 8, 128), F32),
        vm((2 * K, 128), F32),
        sem((8,)), sem((PD,)),
        sem((nz,)), sem((nz,)), sem((2 * nz,)), sem((nz,)), sem((nz,)),
        sem((np_,)), sem((np_,)), sem((nz,)), sem((nz,)),
        sem((np_,)), sem((np_,)), sem((np_,)), sem((np_,)),
        sem((np_,)), sem((np_,)), sem((2,)), sem(()), sem(()),
    ]
    any_spec = pl.BlockSpec(memory_space=pltpu.MemorySpace.HBM)
    vmem_spec = pl.BlockSpec(memory_space=pltpu.VMEM)
    out = jax.ShapeDtypeStruct((PD, 2, W), F32)
    return pl.pallas_call(
        kernel,
        out_shape=(out, out),
        in_specs=[any_spec] * 9,
        out_specs=(vmem_spec, vmem_spec),
        scratch_shapes=scratch,
        compiler_params=pltpu.CompilerParams(
            collective_id=0, has_side_effects=True, vmem_limit_bytes=66_000_000
        ),
    )(*args)


def solution(mesh):
    return jax.shard_map(
        on_device,
        mesh=mesh,
        in_specs=(
            P("patch", "rhs", None),
            P("patch", None, None, None),
            P("patch", None),
            P("patch", None, None),
            P("patch", None, None),
            P("patch", None),
            P("patch", None, None, None),
            P("patch", None, None),
            P("patch", None, None),
        ),
        out_specs=(P("patch", "rhs", None), P("patch", "rhs", None)),
        check_vma=False,
    )
```

```python
import jax
import jax.numpy as jnp
from jax import lax
from jax.experimental import pallas as pl
from jax.experimental.pallas import tpu as pltpu
from jax.sharding import PartitionSpec as P

F32 = jnp.float32
BF16 = jnp.bfloat16
HIGH = lax.Precision.HIGHEST
MESH = pl.DeviceIdType.MESH
PD, K, W, E, NB, FL = 8, 16, 384, 64, 4, 4
NT = (((1,), (1,)), ((), ()))
NN = (((1,), (0,)), ((), ()))


def dot(a, b, dims=NT, precision=None):
    return lax.dot_general(a, b, dims, precision=precision, preferred_element_type=F32)


def split(x):
    hi = x.astype(BF16)
    return hi, (x - hi.astype(F32)).astype(BF16)


def folded(x):
    return x + pltpu.roll(x, 64, 1)


def lane_of(shape):
    return lax.broadcasted_iota(jnp.int32, shape, 1)


def eliminate(top, *others):
    a = jnp.concatenate((top, *others), axis=0)
    lanes = lane_of(a.shape)
    group = 4
    for base in range(0, K, group):
        columns = [jnp.broadcast_to(a[:, k : k + 1], a.shape) for k in range(base, base + group)]
        for i in range(group):
            k = base + i
            column = columns[i]
            inverse = 1.0 / column[k : k + 1, :]
            scaled = column * inverse
            for j in range(i + 1, group):
                columns[j] = columns[j] - scaled * columns[j][k : k + 1, :]
            a = jnp.where(lanes == k, scaled, a - scaled * a[k : k + 1, :])
    return a[K:]


def packed_grams(stack):
    full = dot(stack, stack)
    full = jnp.concatenate((full, jnp.zeros((4 * K, 128 - 4 * K), F32)), axis=1)

    def half(top, low):
        t = top + low
        t = t + pltpu.roll(t, 128 - K, 1)
        even = (lane_of((8, 128)) // K) % 2 == 0
        return jnp.where(even, t[:8], pltpu.roll(t[8:], K, 1))

    a = half(full[:K], full[K : 2 * K])
    b = half(full[2 * K : 3 * K], full[3 * K :])
    return jnp.where(lane_of((8, 128)) < 4 * K, a, pltpu.roll(b, 4 * K, 1))


def unpacked_grams(total):
    t = jnp.concatenate((total, pltpu.roll(total, 128 - K, 1)), axis=0)
    return t[:, :K], t[:, 2 * K : 3 * K], t[:, 4 * K : 5 * K], t[:, 6 * K : 7 * K]


def far_first():
    order = [(dy, dx, dc) for dy in range(4) for dx in range(4) for dc in range(2)]
    order.remove((0, 0, 0))
    return sorted(order, key=lambda t: -(min(t[0], 4 - t[0]) + min(t[1], 4 - t[1])))


def product_split(left, right):
    rhi, rlo = split(right)
    twice = jnp.concatenate((left, left), axis=1)
    hi = twice.astype(BF16)
    lo = (twice - hi.astype(F32)).astype(BF16)
    t = dot(jnp.concatenate((hi, lo), axis=0), jnp.concatenate((rhi, rlo), axis=0), NN)
    return split(t[:E] + t[E:])


def kernel(
    rhs_h, near_h, nbr_h, up_h, su_h, fl_h, tr_h, sd_h, dn_h,
    both_o,
    rhs_v, near_v, nbr_s, up_v, su_v, fl_s, tr_v, sd_v, dn_v,
    gh, gl, hlh, hrh, sh, sl, wh, wl, d2h, d2l, imh, iml, nf,
    cst, tst, dst, mg, lg, lf, pg, wg, pc, cf,
    local_sem, z_recv, sends, recvs,
):
    me = lax.axis_index("patch")
    z = lax.axis_index("rhs")
    np_, nz = lax.axis_size("patch"), lax.axis_size("rhs")
    left, right = lax.rem(me + np_ - 1, np_), lax.rem(me + 1, np_)
    core, chip = lax.rem(me, 2), me // 2
    cx, cy = lax.rem(chip, 4), chip // 4
    peers = [
        (lax.rem(cy + dy, 4) * 4 + lax.rem(cx + dx, 4)) * 2 + lax.rem(core + dc, 2)
        for dy, dx, dc in far_first()
    ]
    z_order = (4, 3, 5, 2, 6, 1, 7)
    z_peers = [lax.rem(z + d, nz) for d in z_order]

    def load(i, src, dst):
        copy = pltpu.make_async_copy(src, dst, local_sem.at[i])
        copy.start()
        return copy

    c_rhs = load(0, rhs_h, rhs_v)
    barrier = pltpu.get_barrier_semaphore()
    for to in z_peers:
        pl.semaphore_signal(barrier, inc=1, device_id=(me, to), device_id_type=MESH)
    for to in peers:
        pl.semaphore_signal(barrier, inc=1, device_id=(to, z), device_id_type=MESH)
    c_up = load(1, up_h, up_v)
    c_su = load(2, su_h, su_v)
    c_tr = load(5, tr_h, tr_v)
    c_sd = load(6, sd_h, sd_v)
    c_dn = load(7, dn_h, dn_v)
    c_fl = load(4, fl_h, fl_s)
    c_nbr = load(3, nbr_h, nbr_s)
    c_near = load(8, near_h, near_v)

    M, L, PA, WA, PC, ZH, ZL, HL, HR, OL, OR, WL, WR, WLL, WRL = range(15)

    def send(src, dst, kind, device, recv=None):
        pltpu.make_async_remote_copy(
            src_ref=src,
            dst_ref=dst,
            send_sem=sends.at[kind],
            recv_sem=recvs.at[kind] if recv is None else recv,
            device_id=device,
            device_id_type=MESH,
        ).start()

    def handle(ref, kind, recv=None):
        return pltpu.make_async_remote_copy(
            src_ref=ref,
            dst_ref=ref,
            send_sem=sends.at[kind],
            recv_sem=recvs.at[kind] if recv is None else recv,
            device_id=(right, z),
            device_id_type=MESH,
        )

    def spread_patch(buf, kind):
        for to in peers:
            send(buf.at[me], buf.at[me], kind, (to, z))

    def gathered_patch(buf, kind):
        handle(buf.at[pl.ds(0, np_ - 1)], kind).wait_recv()

    def spread_z(buf, kind, recv=None):
        for to in z_peers:
            send(buf.at[z], buf.at[z], kind, (me, to), recv)

    def forward(zz):
        send(gh.at[zz], hlh.at[zz], HL, (right, z))
        send(gh.at[zz], hrh.at[zz], HR, (left, z))

    c_rhs.wait()
    own_hi, own_lo = [], []
    for p in range(PD):
        hi, lo = split(rhs_v[p])
        gh[z, p] = hi
        gl[z, p] = lo
        own_hi.append(hi)
        own_lo.append(lo)
    own_hi = jnp.concatenate(own_hi, axis=1)
    own_lo = jnp.concatenate(own_lo, axis=1)

    pl.semaphore_wait(barrier, np_ + nz - 2)
    spread_z(gh, ZH, z_recv.at[z])
    forward(z)

    c_up.wait()
    c_su.wait()
    for p in range(PD):
        hi, lo = product_split(su_v[p], up_v[p])
        cst[:E, p * W : (p + 1) * W] = hi
        cst[E:, p * W : (p + 1) * W] = lo
    mg[me] = folded(dot(own_hi, cst[...]) + dot(own_lo, cst[...]))
    spread_patch(mg, M)

    def take(d):
        zz = lax.rem(z + d, nz)
        handle(gh.at[zz], ZH, z_recv.at[zz]).wait_recv()
        forward(zz)

    for d in (1, 7, 2, 6):
        take(d)

    c_tr.wait()
    for i in range(2):
        hi, lo = split(jnp.concatenate((tr_v[0, 2 * i], tr_v[0, 2 * i + 1]), axis=1))
        tst[:E, i * 128 : (i + 1) * 128] = hi
        tst[E:, i * 128 : (i + 1) * 128] = lo
    c_sd.wait()
    c_dn.wait()
    for p in range(PD):
        hi, lo = product_split(sd_v[p].T, dn_v[p])
        dst[p, :E] = hi
        dst[p, E:] = lo

    for d in (3, 5, 4):
        take(d)
    spread_z(gl, ZL)

    def assembled(buf, dest, base):
        for zz in range(8):
            for p in range(PD):
                dest[base + p, 2 * zz : 2 * zz + 2, :] = buf[zz, p]

    assembled(gh, sh, PD)

    c_fl.wait()
    src = [fl_s[0, j] for j in range(FL)]
    gathered_patch(mg, M)
    low2 = lane_of((2, 128)) < E
    chosen = jnp.concatenate(
        (jnp.where(low2, mg[src[0]], mg[src[1]]), jnp.where(low2, mg[src[2]], mg[src[3]])), axis=1
    )
    hi, lo = split(chosen)
    lg[z] = folded(dot(hi, tst[...]) + dot(lo, tst[...]))
    spread_z(lg, L)

    handle(hlh, HL).wait_recv()
    assembled(hlh, sh, 0)
    handle(hrh, HR).wait_recv()
    assembled(hrh, sh, 2 * PD)

    c_nbr.wait()
    first = me * PD - PD
    total_patches = np_ * PD
    ids = [
        [
            jnp.minimum(lax.rem(nbr_s[j, p] - first + 2 * total_patches, total_patches), 3 * PD - 1)
            for j in range(NB)
        ]
        for p in range(PD)
    ]
    c_near.wait()

    def near_of(p, field):
        blocks = jnp.concatenate([near_v[p, j] for j in range(NB)], axis=1)
        picked = jnp.concatenate([field[ids[p][j]] for j in range(NB)], axis=1)
        return dot(blocks, picked).T

    def far_of(p, lcat):
        far = dot(lcat, dst[p], NN)
        return far[:K] + far[K:]

    for p in range(PD):
        nf[p] = near_of(p, sh)

    handle(gl.at[pl.ds(0, nz - 1)], ZL).wait_recv()
    assembled(gl, sl, PD)
    mid = pl.ds(PD, PD)
    send(sl.at[mid], sl.at[pl.ds(0, PD)], OL, (right, z))
    send(sl.at[mid], sl.at[pl.ds(2 * PD, PD)], OR, (left, z))

    handle(lg.at[pl.ds(0, nz - 1)], L).wait_recv()
    for zz in range(8):
        lf[2 * zz : 2 * zz + 2, :] = lg[zz]
    local0 = lf[...]
    lcat = jnp.concatenate(split(local0), axis=0)
    for p in range(PD):
        hi, lo = split(nf[p] + far_of(p, lcat))
        wh[PD + p] = hi
        wl[PD + p] = lo

    def joined(base, *refs):
        return jnp.concatenate(
            [jnp.concatenate([ref[base + p] for p in range(PD)], axis=1) for ref in refs], axis=0
        )

    pg[me] = packed_grams(joined(PD, sh, sl, wh, wl))
    spread_patch(pg, PA)
    up_w = dot(joined(PD, wh, wl), cst[...])
    up_w = folded(up_w[:K] + up_w[K:])
    low8 = lane_of((8, 128)) < E
    wg[me] = jnp.where(low8, up_w[:8], up_w[8:])
    spread_patch(wg, WA)
    send(wh.at[mid], wh.at[pl.ds(0, PD)], WL, (right, z))
    send(wh.at[mid], wh.at[pl.ds(2 * PD, PD)], WR, (left, z))
    send(wl.at[mid], wl.at[pl.ds(0, PD)], WLL, (right, z))
    send(wl.at[mid], wl.at[pl.ds(2 * PD, PD)], WRL, (left, z))

    gathered_patch(pg, PA)
    rr, gg, gt, qq = unpacked_grams(jnp.sum(pg[...], axis=0))
    eye = (lax.broadcasted_iota(jnp.int32, (K, K), 0) == lane_of((K, K))).astype(F32)
    a1 = eliminate(0.5 * (gg + gt), rr)
    both = eliminate(rr, gt, eye)
    gtk, inv = both[:K], both[K:]
    aq = dot(a1, qq, NN, HIGH) - gg
    ka = dot(inv, a1, NN, HIGH)
    ag = dot(a1, gtk, NN, HIGH)
    first_co, second_co = 2.0 * eye - ag + dot(aq, ka, NT, HIGH), -a1
    rr1 = rr - dot(a1, gt, NN, HIGH) + dot(aq, a1, NT, HIGH)
    mixer = jnp.concatenate((first_co, first_co, second_co, second_co), axis=1)
    mhi = mixer.astype(BF16).astype(F32)
    mixer = jnp.concatenate((mhi, mixer - mhi), axis=0).astype(BF16)

    gathered_patch(wg, WA)
    for kind, ref, base in (
        (OL, sl, 0), (OR, sl, 2 * PD), (WL, wh, 0), (WR, wh, 2 * PD), (WLL, wl, 0), (WRL, wl, 2 * PD)
    ):
        handle(ref.at[pl.ds(base, PD)], kind).wait_recv()

    us = [wg[src[j]] for j in range(FL)]
    rs = [pltpu.roll(u, E, 1) for u in us]
    chosen = jnp.concatenate(
        (
            jnp.concatenate((jnp.where(low8, us[0], rs[1]), jnp.where(low8, rs[0], us[1])), axis=0),
            jnp.concatenate((jnp.where(low8, us[2], rs[3]), jnp.where(low8, rs[2], us[3])), axis=0),
        ),
        axis=1,
    )
    hi, lo = split(chosen)
    local_w = folded(dot(hi, tst[...]) + dot(lo, tst[...]))
    local2 = dot(first_co, local0, NN, HIGH) + dot(second_co, local_w, NN, HIGH)
    lcat = jnp.concatenate(split(local2), axis=0)

    for i in range(3 * PD):
        t = dot(mixer, jnp.concatenate((sh[i], sl[i], wh[i], wl[i]), axis=0), NN)
        hi, lo = split(t[:K] + t[K:])
        d2h[i] = hi
        if PD <= i < 2 * PD:
            d2l[i - PD] = lo

    for p in range(PD):
        hi, lo = split(near_of(p, d2h) + far_of(p, lcat))
        imh[p] = hi
        iml[p] = lo

    wide = [jnp.concatenate([ref[b + p] for p in range(PD)], axis=1) for ref, b in ((d2h, PD), (d2l, 0), (imh, 0), (iml, 0))]
    pc[me] = packed_grams(jnp.concatenate(wide, axis=0))
    spread_patch(pc, PC)

    cf[0:K, 0:K] = a1
    cf[K : 2 * K, 0:K] = rr1
    mine_a1, mine_rr1 = cf[pl.ds(2 * z, 2), 0:K], cf[pl.ds(K + 2 * z, 2), 0:K]
    cf[2 * K : 3 * K, 0:K] = eye
    mine_eye = cf[pl.ds(2 * K + 2 * z, 2), 0:K]
    none = jnp.zeros((2, K), F32)
    coeffs = jnp.concatenate(
        (
            jnp.concatenate((mine_a1, mine_a1, none, none), axis=1),
            jnp.concatenate((mine_eye, mine_eye, -mine_a1, -mine_a1), axis=1),
        ),
        axis=0,
    )
    chi = coeffs.astype(BF16).astype(F32)
    coeffs = jnp.concatenate((chi, coeffs - chi), axis=0).astype(BF16)
    for p in range(PD):
        q = PD + p
        t = dot(coeffs, jnp.concatenate((sh[q], sl[q], wh[q], wl[q]), axis=0), NN)
        both_o[p] = t[:4] + t[4:]
    rows8 = jnp.concatenate((mine_rr1,) * 4, axis=0)
    row8 = lax.broadcasted_iota(jnp.int32, (8, 4 * K), 0)
    lane8 = lane_of((8, 4 * K)) < 2 * K
    is_sol = lax.rem(row8, 4) < 2
    sign = jnp.where(is_sol, jnp.where(lane8, 1.0, 0.0), jnp.where(lane8, 0.0, -1.0))

    gathered_patch(pc, PC)
    _, gg, gt, _ = unpacked_grams(jnp.sum(pc[...], axis=0))
    a2 = eliminate(0.5 * (gg + gt), rows8)
    a2 = jnp.concatenate((a2, a2, a2, a2), axis=1)
    chi = a2.astype(BF16).astype(F32)
    coeffs = (jnp.where(row8 < 4, chi, a2 - chi) * sign).astype(BF16)
    for p in range(PD):
        t = dot(coeffs, jnp.concatenate((d2h[PD + p], d2l[p], imh[p], iml[p]), axis=0), NN)
        both_o[p] += t[:4] + t[4:]

    for ref, kind in ((mg, M), (pg, PA), (wg, WA), (pc, PC)):
        handle(ref.at[pl.ds(0, np_ - 1)], kind).wait_send()
    for ref, kind in ((lg, L), (gh, ZH), (gl, ZL)):
        handle(ref.at[pl.ds(0, nz - 1)], kind).wait_send()
    for ref, kind in ((hlh, HL), (hrh, HR)):
        handle(ref, kind).wait_send()
    for ref, kind in ((sl, OL), (sl, OR), (wh, WL), (wh, WR), (wl, WLL), (wl, WRL)):
        handle(ref.at[mid], kind).wait_send()


def on_device(*args):
    args = list(args)
    args[2] = args[2].T
    args[8] = jnp.swapaxes(args[8], 1, 2)
    args = [pltpu.with_memory_space_constraint(x, pltpu.HBM) for x in args]
    np_, nz = lax.axis_size("patch"), lax.axis_size("rhs")
    vm = pltpu.VMEM
    sem = pltpu.SemaphoreType.DMA
    chunks = vm((nz, PD, 2, W), BF16)
    three = vm((3 * PD, K, W), BF16)
    one = vm((PD, K, W), BF16)
    message = vm((np_, 8, 128), F32)
    scratch = [
        vm((PD, 2, W), F32),
        vm((PD, NB, W, W), BF16),
        pltpu.SMEM((NB, PD), jnp.int32),
        vm((PD, E, W), F32),
        vm((PD, E, E), F32),
        pltpu.SMEM((1, FL), jnp.int32),
        vm((1, FL, E, E), F32),
        vm((PD, E, E), F32),
        vm((PD, E, W), F32),
        chunks, chunks, chunks, chunks,
        three, three, three, three, three, one, one, one,
        vm((PD, K, W), F32),
        vm((2 * E, PD * W), BF16),
        vm((2 * E, FL * E), BF16),
        vm((PD, 2 * E, W), BF16),
        vm((np_, 2, 128), F32),
        vm((nz, 2, 128), F32),
        vm((K, 128), F32),
        message, message, message,
        vm((3 * K, 128), F32),
        sem((9,)), sem((nz,)), sem((15,)), sem((15,)),
    ]
    out = pl.pallas_call(
        kernel,
        out_shape=pltpu.VMEM((PD, 4, W), F32),
        in_specs=[pl.BlockSpec(memory_space=pltpu.MemorySpace.HBM)] * 9,
        out_specs=pl.BlockSpec(memory_space=pltpu.VMEM),
        scratch_shapes=scratch,
        compiler_params=pltpu.CompilerParams(
            collective_id=0, has_side_effects=True, vmem_limit_bytes=60_000_000
        ),
    )(*args)
    return out[:, :2], out[:, 2:]


def solution(mesh):
    return jax.shard_map(
        on_device,
        mesh=mesh,
        in_specs=(
            P("patch", "rhs", None),
            P("patch", None, None, None),
            P("patch", None),
            P("patch", None, None),
            P("patch", None, None),
            P("patch", None),
            P("patch", None, None, None),
            P("patch", None, None),
            P("patch", None, None),
        ),
        out_specs=(P("patch", "rhs", None), P("patch", "rhs", None)),
        check_vma=False,
    )
```

```python
import jax
import jax.numpy as jnp
from jax import lax
from jax.experimental import pallas as pl
from jax.experimental.pallas import tpu as pltpu
from jax.sharding import PartitionSpec as P

F32 = jnp.float32
BF16 = jnp.bfloat16
HIGH = lax.Precision.HIGHEST
MESH = pl.DeviceIdType.MESH
PD, K, W, E, NB, FL = 8, 16, 384, 64, 4, 4
NT = (((1,), (1,)), ((), ()))
NN = (((1,), (0,)), ((), ()))


def dot(a, b, dims=NT, precision=None):
    return lax.dot_general(a, b, dims, precision=precision, preferred_element_type=F32)


def split(x):
    hi = x.astype(BF16)
    return hi, (x - hi.astype(F32)).astype(BF16)


def folded(x):
    return x + pltpu.roll(x, 64, 1)


def lane_of(shape):
    return lax.broadcasted_iota(jnp.int32, shape, 1)


def eliminate(top, *others):
    a = jnp.concatenate((top, *others), axis=0)
    lanes = lane_of(a.shape)
    group = 4
    for base in range(0, K, group):
        columns = [jnp.broadcast_to(a[:, k : k + 1], a.shape) for k in range(base, base + group)]
        for i in range(group):
            k = base + i
            column = columns[i]
            inverse = 1.0 / column[k : k + 1, :]
            scaled = column * inverse
            for j in range(i + 1, group):
                columns[j] = columns[j] - scaled * columns[j][k : k + 1, :]
            a = jnp.where(lanes == k, scaled, a - scaled * a[k : k + 1, :])
    return a[K:]


def packed_grams(rows, high, low):
    full = dot(rows, high) + dot(rows, low)
    a = full[:K] + full[K : 2 * K]
    b = full[2 * K : 3 * K] + full[3 * K :]
    return jnp.concatenate((a[:8], a[8:], b[:8], b[8:]), axis=1)


def unpacked_grams(total):
    def at(lane):
        return pltpu.roll(total, 128 - lane, 1) if lane else total

    def block(lane):
        return jnp.concatenate((at(lane), at(lane + 2 * K)), axis=0)[:, :K]

    return block(0), block(K), block(4 * K), block(5 * K)


def far_first():
    order = [(dy, dx, dc) for dy in range(4) for dx in range(4) for dc in range(2)]
    order.remove((0, 0, 0))
    return sorted(order, key=lambda t: -(min(t[0], 4 - t[0]) + min(t[1], 4 - t[1])))


def product_split(left, right):
    rhi, rlo = split(right)
    twice = jnp.concatenate((left, left), axis=1)
    hi = twice.astype(BF16)
    lo = (twice - hi.astype(F32)).astype(BF16)
    t = dot(jnp.concatenate((hi, lo), axis=0), jnp.concatenate((rhi, rlo), axis=0), NN)
    return split(t[:E] + t[E:])


def kernel(
    rhs_h, near_h, nbr_h, up_h, su_h, fl_h, tr_h, sd_h, dn_h,
    both_o,
    rhs_v, near_v, nbr_s, up_v, su_v, fl_s, tr_v, sd_v, dn_v,
    gh, gl, hlh, hrh, sh, sl, wh, wl, d2h, d2w, imh, iml, nf,
    cst, tst, dst, mg, lg, lf, pg, wg, pc, cf,
    local_sem, z_recv, sends, recvs,
):
    me = lax.axis_index("patch")
    z = lax.axis_index("rhs")
    np_, nz = lax.axis_size("patch"), lax.axis_size("rhs")
    left, right = lax.rem(me + np_ - 1, np_), lax.rem(me + 1, np_)
    core, chip = lax.rem(me, 2), me // 2
    cx, cy = lax.rem(chip, 4), chip // 4
    peers = [
        (lax.rem(cy + dy, 4) * 4 + lax.rem(cx + dx, 4)) * 2 + lax.rem(core + dc, 2)
        for dy, dx, dc in far_first()
    ]
    z_order = (4, 3, 5, 2, 6, 1, 7)
    z_peers = [lax.rem(z + d, nz) for d in z_order]

    def load(i, src, dst):
        copy = pltpu.make_async_copy(src, dst, local_sem.at[i])
        copy.start()
        return copy

    c_rhs = load(0, rhs_h, rhs_v)
    barrier = pltpu.get_barrier_semaphore()
    for to in z_peers:
        pl.semaphore_signal(barrier, inc=1, device_id=(me, to), device_id_type=MESH)
    for to in peers:
        pl.semaphore_signal(barrier, inc=1, device_id=(to, z), device_id_type=MESH)
    c_up = load(1, up_h, up_v)
    c_su = load(2, su_h, su_v)
    c_tr = load(5, tr_h, tr_v)
    c_sd = load(6, sd_h, sd_v)
    c_dn = load(7, dn_h, dn_v)
    c_fl = load(4, fl_h, fl_s)
    c_nbr = load(3, nbr_h, nbr_s)
    M, L, PA, WA, PC, ZH, ZL, HL, HR, OL, OR, WL, WR, WLL, WRL = range(15)

    def send(src, dst, kind, device, recv=None):
        pltpu.make_async_remote_copy(
            src_ref=src,
            dst_ref=dst,
            send_sem=sends.at[kind],
            recv_sem=recvs.at[kind] if recv is None else recv,
            device_id=device,
            device_id_type=MESH,
        ).start()

    def handle(ref, kind, recv=None):
        return pltpu.make_async_remote_copy(
            src_ref=ref,
            dst_ref=ref,
            send_sem=sends.at[kind],
            recv_sem=recvs.at[kind] if recv is None else recv,
            device_id=(right, z),
            device_id_type=MESH,
        )

    def spread_patch(buf, kind):
        for to in peers:
            send(buf.at[me], buf.at[me], kind, (to, z))

    def gathered_patch(buf, kind):
        handle(buf.at[pl.ds(0, np_ - 1)], kind).wait_recv()

    def spread_z(buf, kind, recv=None):
        for to in z_peers:
            send(buf.at[z], buf.at[z], kind, (me, to), recv)

    def forward(zz):
        send(gh.at[zz], hlh.at[zz], HL, (right, z))
        send(gh.at[zz], hrh.at[zz], HR, (left, z))

    c_rhs.wait()
    own_hi, own_lo = [], []
    for p in range(PD):
        hi, lo = split(rhs_v[p])
        gh[z, p] = hi
        gl[z, p] = lo
        own_hi.append(hi)
        own_lo.append(lo)
    own_hi = jnp.concatenate(own_hi, axis=1)
    own_lo = jnp.concatenate(own_lo, axis=1)

    pl.semaphore_wait(barrier, np_ + nz - 2)
    spread_z(gh, ZH, z_recv.at[z])
    forward(z)

    c_up.wait()
    c_su.wait()
    c_near = load(8, near_h, near_v)
    for p in range(PD):
        hi, lo = product_split(su_v[p], up_v[p])
        cst[:E, p * W : (p + 1) * W] = hi
        cst[E:, p * W : (p + 1) * W] = lo
    mg[me] = folded(dot(own_hi, cst[...]) + dot(own_lo, cst[...]))
    spread_patch(mg, M)

    def take(d):
        zz = lax.rem(z + d, nz)
        handle(gh.at[zz], ZH, z_recv.at[zz]).wait_recv()
        forward(zz)

    c_tr.wait()
    for i in range(2):
        hi, lo = split(jnp.concatenate((tr_v[0, 2 * i], tr_v[0, 2 * i + 1]), axis=1))
        tst[:E, i * 128 : (i + 1) * 128] = hi
        tst[E:, i * 128 : (i + 1) * 128] = lo

    for d in (1, 7, 2, 6, 3, 5, 4):
        take(d)

    def assembled(buf, dest, base):
        for zz in range(8):
            for p in range(PD):
                dest[base + p, 2 * zz : 2 * zz + 2, :] = buf[zz, p]

    c_fl.wait()
    src = [fl_s[0, j] for j in range(FL)]
    gathered_patch(mg, M)
    low2 = lane_of((2, 128)) < E
    chosen = jnp.concatenate(
        (jnp.where(low2, mg[src[0]], mg[src[1]]), jnp.where(low2, mg[src[2]], mg[src[3]])), axis=1
    )
    hi, lo = split(chosen)
    lg[z] = folded(dot(hi, tst[...]) + dot(lo, tst[...]))
    spread_z(lg, L)
    spread_z(gl, ZL)

    assembled(gh, sh, PD)
    c_sd.wait()
    c_dn.wait()
    for p in range(PD):
        hi, lo = product_split(sd_v[p].T, dn_v[p])
        dst[p, :E] = hi
        dst[p, E:] = lo

    c_near.wait()
    for p in range(PD):
        nf[p] = dot(near_v[p, 0], sh[PD + p]).T

    handle(hlh, HL).wait_recv()
    assembled(hlh, sh, 0)
    handle(hrh, HR).wait_recv()
    assembled(hrh, sh, 2 * PD)

    c_nbr.wait()
    first = me * PD - PD
    total_patches = np_ * PD
    ids = [
        [
            jnp.minimum(lax.rem(nbr_s[j, p] - first + 2 * total_patches, total_patches), 3 * PD - 1)
            for j in range(NB)
        ]
        for p in range(PD)
    ]

    def near_of(p, field, start):
        blocks = jnp.concatenate([near_v[p, j] for j in range(start, NB)], axis=1)
        picked = jnp.concatenate([field[ids[p][j]] for j in range(start, NB)], axis=1)
        return dot(blocks, picked).T

    def far_of(p, lcat):
        far = dot(lcat, dst[p], NN)
        return far[:K] + far[K:]

    for p in range(PD):
        nf[p] += near_of(p, sh, 1)

    handle(gl.at[pl.ds(0, nz - 1)], ZL).wait_recv()
    assembled(gl, sl, PD)
    mid = pl.ds(PD, PD)
    send(sl.at[mid], sl.at[pl.ds(0, PD)], OL, (right, z))
    send(sl.at[mid], sl.at[pl.ds(2 * PD, PD)], OR, (left, z))

    handle(lg.at[pl.ds(0, nz - 1)], L).wait_recv()
    for zz in range(8):
        lf[2 * zz : 2 * zz + 2, :] = lg[zz]
    local0 = lf[...]
    lcat = jnp.concatenate(split(local0), axis=0)
    for p in range(PD):
        hi, lo = split(nf[p] + far_of(p, lcat))
        wh[PD + p] = hi
        wl[PD + p] = lo

    def joined(base, *refs):
        return jnp.concatenate(
            [jnp.concatenate([ref[base + p] for p in range(PD)], axis=1) for ref in refs], axis=0
        )

    pg[me] = packed_grams(joined(PD, sh, sl, wh, wl), joined(PD, wh, sh), joined(PD, wl, sl))
    spread_patch(pg, PA)
    up_w = dot(joined(PD, wh, wl), cst[...])
    up_w = folded(up_w[:K] + up_w[K:])
    low8 = lane_of((8, 128)) < E
    wg[me] = jnp.where(low8, up_w[:8], up_w[8:])
    spread_patch(wg, WA)
    send(wh.at[mid], wh.at[pl.ds(0, PD)], WL, (right, z))
    send(wh.at[mid], wh.at[pl.ds(2 * PD, PD)], WR, (left, z))
    send(wl.at[mid], wl.at[pl.ds(0, PD)], WLL, (right, z))
    send(wl.at[mid], wl.at[pl.ds(2 * PD, PD)], WRL, (left, z))

    gathered_patch(pg, PA)
    gg, rr, qq, gt = unpacked_grams(jnp.sum(pg[...], axis=0))
    eye = (lax.broadcasted_iota(jnp.int32, (K, K), 0) == lane_of((K, K))).astype(F32)
    a1 = eliminate(0.5 * (gg + gt), rr)
    inv = eliminate(rr, eye)
    blank = jnp.zeros((2 * K, K), F32)
    aq = dot(a1, qq, NN, HIGH) - gg
    ag = dot(a1, gg, NT, HIGH)
    ka = dot(inv, a1, NN, HIGH)
    row16, lane64 = lax.broadcasted_iota(jnp.int32, (K, 4 * K), 0), lane_of((K, 4 * K))
    twice = jnp.where((lane64 == row16) | (lane64 == row16 + K), 2.0, 0.0)
    minus = jnp.concatenate((jnp.zeros((K, 2 * K), F32), -a1, -a1), axis=1)
    first = dot(aq, jnp.concatenate((ka, ka, blank), axis=0), NT, HIGH)
    first = first - dot(ag, jnp.concatenate((inv, inv, blank), axis=0), NT, HIGH) + twice
    mixer = first + minus
    first_co, second_co = first[:, :K], -a1
    rr1 = rr - ag + dot(aq, a1, NT, HIGH)
    mhi = mixer.astype(BF16).astype(F32)
    mixer = jnp.concatenate((mhi, mixer - mhi), axis=0).astype(BF16)

    gathered_patch(wg, WA)
    for kind, ref, base in (
        (OL, sl, 0), (OR, sl, 2 * PD), (WL, wh, 0), (WR, wh, 2 * PD), (WLL, wl, 0), (WRL, wl, 2 * PD)
    ):
        handle(ref.at[pl.ds(base, PD)], kind).wait_recv()

    us = [wg[src[j]] for j in range(FL)]
    rs = [pltpu.roll(u, E, 1) for u in us]
    chosen = jnp.concatenate(
        (
            jnp.concatenate((jnp.where(low8, us[0], rs[1]), jnp.where(low8, rs[0], us[1])), axis=0),
            jnp.concatenate((jnp.where(low8, us[2], rs[3]), jnp.where(low8, rs[2], us[3])), axis=0),
        ),
        axis=1,
    )
    hi, lo = split(chosen)
    local_w = folded(dot(hi, tst[...]) + dot(lo, tst[...]))
    local2 = dot(first_co, local0, NN, HIGH) + dot(second_co, local_w, NN, HIGH)
    lcat = jnp.concatenate(split(local2), axis=0)

    for i in range(3 * PD):
        t = dot(mixer, jnp.concatenate((sh[i], sl[i], wh[i], wl[i]), axis=0), NN)
        hi, lo = split(t[:K] + t[K:])
        d2h[i] = hi
        if PD <= i < 2 * PD:
            d2w[i] = lo

    for p in range(PD):
        hi, lo = split(near_of(p, d2h, 0) + far_of(p, lcat))
        imh[p] = hi
        iml[p] = lo

    def crossed(base_a, ah, al, base_b, bh, bl):
        rows = jnp.concatenate((joined(base_a, ah), joined(base_a, al)), axis=0)
        t = dot(rows, joined(base_b, bh)) + dot(rows, joined(base_b, bl))
        return t[:K] + t[K:]

    half = crossed(PD, d2h, d2w, 0, imh, iml) + crossed(0, imh, iml, PD, d2h, d2w)
    half = 0.5 * half
    pc[me] = jnp.concatenate([half[2 * i : 2 * i + 2] for i in range(8)], axis=1)
    spread_patch(pc, PC)

    cf[0:K, 0:K] = a1
    cf[K : 2 * K, 0:K] = rr1
    mine_a1, mine_rr1 = cf[pl.ds(2 * z, 2), 0:K], cf[pl.ds(K + 2 * z, 2), 0:K]
    cf[2 * K : 3 * K, 0:K] = eye
    mine_eye = cf[pl.ds(2 * K + 2 * z, 2), 0:K]
    none = jnp.zeros((2, K), F32)
    coeffs = jnp.concatenate(
        (
            jnp.concatenate((mine_a1, mine_a1, none, none), axis=1),
            jnp.concatenate((mine_eye, mine_eye, -mine_a1, -mine_a1), axis=1),
        ),
        axis=0,
    )
    chi = coeffs.astype(BF16).astype(F32)
    coeffs = jnp.concatenate((chi, coeffs - chi), axis=0).astype(BF16)
    for p in range(PD):
        q = PD + p
        t = dot(coeffs, jnp.concatenate((sh[q], sl[q], wh[q], wl[q]), axis=0), NN)
        both_o[p] = t[:4] + t[4:]
    rows8 = jnp.concatenate((mine_rr1,) * 4, axis=0)
    row8 = lax.broadcasted_iota(jnp.int32, (8, 4 * K), 0)
    lane8 = lane_of((8, 4 * K)) < 2 * K
    is_sol = lax.rem(row8, 4) < 2
    sign = jnp.where(is_sol, jnp.where(lane8, 1.0, 0.0), jnp.where(lane8, 0.0, -1.0))

    gathered_patch(pc, PC)
    total = jnp.sum(pc[...], axis=0)
    moved = [total] + [pltpu.roll(total, 128 - K * i, 1) for i in range(1, 8)]
    a2 = eliminate(jnp.concatenate(moved, axis=0)[:, :K], rows8)
    a2 = jnp.concatenate((a2, a2, a2, a2), axis=1)
    chi = a2.astype(BF16).astype(F32)
    coeffs = (jnp.where(row8 < 4, chi, a2 - chi) * sign).astype(BF16)
    for p in range(PD):
        t = dot(coeffs, jnp.concatenate((d2h[PD + p], d2w[PD + p], imh[p], iml[p]), axis=0), NN)
        both_o[p] += t[:4] + t[4:]

    for ref, kind in ((mg, M), (pg, PA), (wg, WA), (pc, PC)):
        handle(ref.at[pl.ds(0, np_ - 1)], kind).wait_send()
    for ref, kind in ((lg, L), (gh, ZH), (gl, ZL)):
        handle(ref.at[pl.ds(0, nz - 1)], kind).wait_send()
    for ref, kind in ((hlh, HL), (hrh, HR)):
        handle(ref, kind).wait_send()
    for ref, kind in ((sl, OL), (sl, OR), (wh, WL), (wh, WR), (wl, WLL), (wl, WRL)):
        handle(ref.at[mid], kind).wait_send()


def on_device(*args):
    args = list(args)
    args[2] = args[2].T
    args[8] = jnp.swapaxes(args[8], 1, 2)
    args = [pltpu.with_memory_space_constraint(x, pltpu.HBM) for x in args]
    np_, nz = lax.axis_size("patch"), lax.axis_size("rhs")
    vm = pltpu.VMEM
    sem = pltpu.SemaphoreType.DMA
    chunks = vm((nz, PD, 2, W), BF16)
    three = vm((3 * PD, K, W), BF16)
    one = vm((PD, K, W), BF16)
    message = vm((np_, 8, 128), F32)
    scratch = [
        vm((PD, 2, W), F32),
        vm((PD, NB, W, W), BF16),
        pltpu.SMEM((NB, PD), jnp.int32),
        vm((PD, E, W), F32),
        vm((PD, E, E), F32),
        pltpu.SMEM((1, FL), jnp.int32),
        vm((1, FL, E, E), F32),
        vm((PD, E, E), F32),
        vm((PD, E, W), F32),
        chunks, chunks, chunks, chunks,
        three, three, three, three, three, three, one, one,
        vm((PD, K, W), F32),
        vm((2 * E, PD * W), BF16),
        vm((2 * E, FL * E), BF16),
        vm((PD, 2 * E, W), BF16),
        vm((np_, 2, 128), F32),
        vm((nz, 2, 128), F32),
        vm((K, 128), F32),
        message, message,
        vm((np_, 2, 128), F32),
        vm((3 * K, 128), F32),
        sem((9,)), sem((nz,)), sem((15,)), sem((15,)),
    ]
    out = pl.pallas_call(
        kernel,
        out_shape=pltpu.VMEM((PD, 4, W), F32),
        in_specs=[pl.BlockSpec(memory_space=pltpu.MemorySpace.HBM)] * 9,
        out_specs=pl.BlockSpec(memory_space=pltpu.VMEM),
        scratch_shapes=scratch,
        compiler_params=pltpu.CompilerParams(
            collective_id=0, has_side_effects=True, vmem_limit_bytes=60_000_000
        ),
    )(*args)
    return out[:, :2], out[:, 2:]


def solution(mesh):
    return jax.shard_map(
        on_device,
        mesh=mesh,
        in_specs=(
            P("patch", "rhs", None),
            P("patch", None, None, None),
            P("patch", None),
            P("patch", None, None),
            P("patch", None, None),
            P("patch", None),
            P("patch", None, None, None),
            P("patch", None, None),
            P("patch", None, None),
        ),
        out_specs=(P("patch", "rhs", None), P("patch", "rhs", None)),
        check_vma=False,
    )
```

```python
import jax
import jax.numpy as jnp
from jax import lax
from jax.experimental import pallas as pl
from jax.experimental.pallas import tpu as pltpu
from jax.sharding import PartitionSpec as P

F32 = jnp.float32
BF16 = jnp.bfloat16
HIGH = lax.Precision.HIGHEST
MESH = pl.DeviceIdType.MESH
PD, K, W, E, NB, FL = 8, 16, 384, 64, 4, 4
NT = (((1,), (1,)), ((), ()))
NN = (((1,), (0,)), ((), ()))


def dot(a, b, dims=NT, precision=None):
    return lax.dot_general(a, b, dims, precision=precision, preferred_element_type=F32)


def split(x):
    hi = x.astype(BF16)
    return hi, (x - hi.astype(F32)).astype(BF16)


def folded(x):
    return x + pltpu.roll(x, 64, 1)


def lane_of(shape):
    return lax.broadcasted_iota(jnp.int32, shape, 1)


def eliminate(top, *others):
    a = jnp.concatenate((top, *others), axis=0)
    lanes = lane_of(a.shape)
    group = 4
    for base in range(0, K, group):
        columns = [jnp.broadcast_to(a[:, k : k + 1], a.shape) for k in range(base, base + group)]
        for i in range(group):
            k = base + i
            column = columns[i]
            inverse = 1.0 / column[k : k + 1, :]
            scaled = column * inverse
            for j in range(i + 1, group):
                columns[j] = columns[j] - scaled * columns[j][k : k + 1, :]
            a = jnp.where(lanes == k, scaled, a - scaled * a[k : k + 1, :])
    return a[K:]


def packed_grams(rows, high, low):
    full = dot(rows, high) + dot(rows, low)
    a = full[:K] + full[K : 2 * K]
    b = full[2 * K : 3 * K] + full[3 * K :]
    return jnp.concatenate((a[:8], a[8:], b[:8], b[8:]), axis=1)


def unpacked_grams(total):
    def at(lane):
        return pltpu.roll(total, 128 - lane, 1) if lane else total

    def block(lane):
        return jnp.concatenate((at(lane), at(lane + 2 * K)), axis=0)[:, :K]

    return block(0), block(K), block(4 * K), block(5 * K)


def far_first():
    order = [(dy, dx, dc) for dy in range(4) for dx in range(4) for dc in range(2)]
    order.remove((0, 0, 0))
    return sorted(order, key=lambda t: -(min(t[0], 4 - t[0]) + min(t[1], 4 - t[1])))


def product_split(left, right):
    rhi, rlo = split(right)
    twice = jnp.concatenate((left, left), axis=1)
    hi = twice.astype(BF16)
    lo = (twice - hi.astype(F32)).astype(BF16)
    t = dot(jnp.concatenate((hi, lo), axis=0), jnp.concatenate((rhi, rlo), axis=0), NN)
    return split(t[:E] + t[E:])


def kernel(
    rhs_h, near_h, nbr_h, up_h, su_h, fl_h, tr_h, sd_h, dn_h,
    both_o,
    rhs_v, near_v, nbr_s, up_v, su_v, fl_s, tr_v, sd_v, dn_v,
    gh, gl, hlh, hrh, sh, sl, wh, wl, d2h, d2w, imh, iml, nf,
    cst, tst, dst, mg, lg, lf, pg, wg, pc, cf,
    local_sem, z_recv, sends, recvs,
):
    me = lax.axis_index("patch")
    z = lax.axis_index("rhs")
    np_, nz = lax.axis_size("patch"), lax.axis_size("rhs")
    left, right = lax.rem(me + np_ - 1, np_), lax.rem(me + 1, np_)
    core, chip = lax.rem(me, 2), me // 2
    cx, cy = lax.rem(chip, 4), chip // 4
    peers = [
        (lax.rem(cy + dy, 4) * 4 + lax.rem(cx + dx, 4)) * 2 + lax.rem(core + dc, 2)
        for dy, dx, dc in far_first()
    ]
    z_order = (4, 3, 5, 2, 6, 1, 7)
    z_peers = [lax.rem(z + d, nz) for d in z_order]

    def load(i, src, dst):
        copy = pltpu.make_async_copy(src, dst, local_sem.at[i])
        copy.start()
        return copy

    c_rhs = load(0, rhs_h, rhs_v)
    barrier = pltpu.get_barrier_semaphore()
    for to in z_peers:
        pl.semaphore_signal(barrier, inc=1, device_id=(me, to), device_id_type=MESH)
    for to in peers:
        pl.semaphore_signal(barrier, inc=1, device_id=(to, z), device_id_type=MESH)
    c_up = load(1, up_h, up_v)
    c_su = load(2, su_h, su_v)
    c_tr = load(5, tr_h, tr_v)
    c_sd = load(6, sd_h, sd_v)
    c_dn = load(7, dn_h, dn_v)
    c_fl = load(4, fl_h, fl_s)
    c_nbr = load(3, nbr_h, nbr_s)
    M, L, PA, WA, PC, ZH, ZL, HL, HR, OL, OR, WL, WR, WLL, WRL = range(15)

    def send(src, dst, kind, device, recv=None):
        pltpu.make_async_remote_copy(
            src_ref=src,
            dst_ref=dst,
            send_sem=sends.at[kind],
            recv_sem=recvs.at[kind] if recv is None else recv,
            device_id=device,
            device_id_type=MESH,
        ).start()

    def handle(ref, kind, recv=None):
        return pltpu.make_async_remote_copy(
            src_ref=ref,
            dst_ref=ref,
            send_sem=sends.at[kind],
            recv_sem=recvs.at[kind] if recv is None else recv,
            device_id=(right, z),
            device_id_type=MESH,
        )

    def spread_patch(buf, kind):
        for to in peers:
            send(buf.at[me], buf.at[me], kind, (to, z))

    def gathered_patch(buf, kind):
        handle(buf.at[pl.ds(0, np_ - 1)], kind).wait_recv()

    def spread_z(buf, kind, recv=None):
        for to in z_peers:
            send(buf.at[z], buf.at[z], kind, (me, to), recv)

    def forward(zz):
        send(gh.at[zz], hlh.at[zz], HL, (right, z))
        send(gh.at[zz], hrh.at[zz], HR, (left, z))

    c_rhs.wait()
    own_hi, own_lo = [], []
    for p in range(PD):
        hi, lo = split(rhs_v[p])
        gh[z, p] = hi
        gl[z, p] = lo
        own_hi.append(hi)
        own_lo.append(lo)
    own_hi = jnp.concatenate(own_hi, axis=1)
    own_lo = jnp.concatenate(own_lo, axis=1)

    pl.semaphore_wait(barrier, np_ + nz - 2)
    spread_z(gh, ZH, z_recv.at[z])
    forward(z)

    c_up.wait()
    c_su.wait()
    c_near = load(8, near_h, near_v)
    for p in range(PD):
        hi, lo = product_split(su_v[p], up_v[p])
        cst[:E, p * W : (p + 1) * W] = hi
        cst[E:, p * W : (p + 1) * W] = lo
    mg[me] = folded(dot(own_hi, cst[...]) + dot(own_lo, cst[...]))
    spread_patch(mg, M)

    def take(d):
        zz = lax.rem(z + d, nz)
        handle(gh.at[zz], ZH, z_recv.at[zz]).wait_recv()
        forward(zz)

    c_tr.wait()
    for i in range(2):
        hi, lo = split(jnp.concatenate((tr_v[0, 2 * i], tr_v[0, 2 * i + 1]), axis=1))
        tst[:E, i * 128 : (i + 1) * 128] = hi
        tst[E:, i * 128 : (i + 1) * 128] = lo

    for d in (1, 7, 2, 6, 3, 5, 4):
        take(d)

    def assembled(buf, dest, base):
        for zz in range(8):
            for p in range(PD):
                dest[base + p, 2 * zz : 2 * zz + 2, :] = buf[zz, p]

    c_fl.wait()
    src = [fl_s[0, j] for j in range(FL)]
    spread_z(gl, ZL)
    gathered_patch(mg, M)
    low2 = lane_of((2, 128)) < E
    chosen = jnp.concatenate(
        (jnp.where(low2, mg[src[0]], mg[src[1]]), jnp.where(low2, mg[src[2]], mg[src[3]])), axis=1
    )
    hi, lo = split(chosen)
    lg[z] = folded(dot(hi, tst[...]) + dot(lo, tst[...]))
    spread_z(lg, L)

    assembled(gh, sh, PD)
    c_sd.wait()
    c_dn.wait()
    for p in range(PD):
        hi, lo = product_split(sd_v[p].T, dn_v[p])
        dst[p, :E] = hi
        dst[p, E:] = lo

    c_near.wait()
    for p in range(PD):
        nf[p] = dot(near_v[p, 0], sh[PD + p]).T

    handle(hlh, HL).wait_recv()
    assembled(hlh, sh, 0)
    handle(hrh, HR).wait_recv()
    assembled(hrh, sh, 2 * PD)

    c_nbr.wait()
    first = me * PD - PD
    total_patches = np_ * PD
    ids = [
        [
            jnp.minimum(lax.rem(nbr_s[j, p] - first + 2 * total_patches, total_patches), 3 * PD - 1)
            for j in range(NB)
        ]
        for p in range(PD)
    ]

    def near_of(p, field, start):
        blocks = jnp.concatenate([near_v[p, j] for j in range(start, NB)], axis=1)
        picked = jnp.concatenate([field[ids[p][j]] for j in range(start, NB)], axis=1)
        return dot(blocks, picked).T if p % 4 != 3 else dot(picked, blocks)

    def far_of(p, lcat):
        far = dot(lcat, dst[p], NN)
        return far[:K] + far[K:]

    for p in range(PD):
        nf[p] += near_of(p, sh, 1)

    handle(gl.at[pl.ds(0, nz - 1)], ZL).wait_recv()
    assembled(gl, sl, PD)
    mid = pl.ds(PD, PD)
    send(sl.at[mid], sl.at[pl.ds(0, PD)], OL, (right, z))
    send(sl.at[mid], sl.at[pl.ds(2 * PD, PD)], OR, (left, z))

    handle(lg.at[pl.ds(0, nz - 1)], L).wait_recv()
    for zz in range(8):
        lf[2 * zz : 2 * zz + 2, :] = lg[zz]
    local0 = lf[...]
    lcat = jnp.concatenate(split(local0), axis=0)
    for p in range(PD):
        hi, lo = split(nf[p] + far_of(p, lcat))
        wh[PD + p] = hi
        wl[PD + p] = lo

    def joined(base, *refs):
        return jnp.concatenate(
            [jnp.concatenate([ref[base + p] for p in range(PD)], axis=1) for ref in refs], axis=0
        )

    pg[me] = packed_grams(joined(PD, sh, sl, wh, wl), joined(PD, wh, sh), joined(PD, wl, sl))
    spread_patch(pg, PA)
    up_w = dot(joined(PD, wh, wl), cst[...])
    up_w = folded(up_w[:K] + up_w[K:])
    low8 = lane_of((8, 128)) < E
    wg[me] = jnp.where(low8, up_w[:8], up_w[8:])
    spread_patch(wg, WA)
    send(wh.at[mid], wh.at[pl.ds(0, PD)], WL, (right, z))
    send(wh.at[mid], wh.at[pl.ds(2 * PD, PD)], WR, (left, z))
    send(wl.at[mid], wl.at[pl.ds(0, PD)], WLL, (right, z))
    send(wl.at[mid], wl.at[pl.ds(2 * PD, PD)], WRL, (left, z))

    gathered_patch(pg, PA)
    gg, rr, qq, gt = unpacked_grams(jnp.sum(pg[...], axis=0))
    eye = (lax.broadcasted_iota(jnp.int32, (K, K), 0) == lane_of((K, K))).astype(F32)
    a1 = eliminate(0.5 * (gg + gt), rr)
    inv = eliminate(rr, eye)
    blank = jnp.zeros((2 * K, K), F32)
    aq = dot(a1, qq, NN, HIGH) - gg
    ag = dot(a1, gg, NT, HIGH)
    ka = dot(inv, a1, NN, HIGH)
    row16, lane64 = lax.broadcasted_iota(jnp.int32, (K, 4 * K), 0), lane_of((K, 4 * K))
    twice = jnp.where((lane64 == row16) | (lane64 == row16 + K), 2.0, 0.0)
    minus = jnp.concatenate((jnp.zeros((K, 2 * K), F32), -a1, -a1), axis=1)
    first = dot(aq, jnp.concatenate((ka, ka, blank), axis=0), NT, HIGH)
    first = first - dot(ag, jnp.concatenate((inv, inv, blank), axis=0), NT, HIGH) + twice
    mixer = first + minus
    first_co, second_co = first[:, :K], -a1
    rr1 = rr - ag + dot(aq, a1, NT, HIGH)
    mhi = mixer.astype(BF16).astype(F32)
    mixer = jnp.concatenate((mhi, mixer - mhi), axis=0).astype(BF16)

    for kind, ref, base in (
        (OL, sl, 0), (OR, sl, 2 * PD), (WL, wh, 0), (WR, wh, 2 * PD), (WLL, wl, 0), (WRL, wl, 2 * PD)
    ):
        handle(ref.at[pl.ds(base, PD)], kind).wait_recv()

    for i in range(3 * PD):
        t = dot(mixer, jnp.concatenate((sh[i], sl[i], wh[i], wl[i]), axis=0), NN)
        hi, lo = split(t[:K] + t[K:])
        d2h[i] = hi
        if PD <= i < 2 * PD:
            d2w[i] = lo

    gathered_patch(wg, WA)
    us = [wg[src[j]] for j in range(FL)]
    rs = [pltpu.roll(u, E, 1) for u in us]
    chosen = jnp.concatenate(
        (
            jnp.concatenate((jnp.where(low8, us[0], rs[1]), jnp.where(low8, rs[0], us[1])), axis=0),
            jnp.concatenate((jnp.where(low8, us[2], rs[3]), jnp.where(low8, rs[2], us[3])), axis=0),
        ),
        axis=1,
    )
    hi, lo = split(chosen)
    local_w = folded(dot(hi, tst[...]) + dot(lo, tst[...]))
    local2 = dot(first_co, local0, NN, HIGH) + dot(second_co, local_w, NN, HIGH)
    lcat = jnp.concatenate(split(local2), axis=0)

    for p in range(PD):
        hi, lo = split(near_of(p, d2h, 0) + far_of(p, lcat))
        imh[p] = hi
        iml[p] = lo

    def crossed(base_a, ah, al, base_b, bh, bl):
        rows = jnp.concatenate((joined(base_a, ah), joined(base_a, al)), axis=0)
        t = dot(rows, joined(base_b, bh)) + dot(rows, joined(base_b, bl))
        return t[:K] + t[K:]

    half = crossed(PD, d2h, d2w, 0, imh, iml) + crossed(0, imh, iml, PD, d2h, d2w)
    half = 0.5 * half
    pc[me] = jnp.concatenate([half[2 * i : 2 * i + 2] for i in range(8)], axis=1)
    spread_patch(pc, PC)

    cf[0:K, 0:K] = a1
    cf[K : 2 * K, 0:K] = rr1
    mine_a1, mine_rr1 = cf[pl.ds(2 * z, 2), 0:K], cf[pl.ds(K + 2 * z, 2), 0:K]
    cf[2 * K : 3 * K, 0:K] = eye
    mine_eye = cf[pl.ds(2 * K + 2 * z, 2), 0:K]
    none = jnp.zeros((2, K), F32)
    coeffs = jnp.concatenate(
        (
            jnp.concatenate((mine_a1, mine_a1, none, none), axis=1),
            jnp.concatenate((mine_eye, mine_eye, -mine_a1, -mine_a1), axis=1),
        ),
        axis=0,
    )
    chi = coeffs.astype(BF16).astype(F32)
    coeffs = jnp.concatenate((chi, coeffs - chi), axis=0).astype(BF16)
    for p in range(PD):
        q = PD + p
        t = dot(coeffs, jnp.concatenate((sh[q], sl[q], wh[q], wl[q]), axis=0), NN)
        both_o[p] = t[:4] + t[4:]
    rows8 = jnp.concatenate((mine_rr1,) * 4, axis=0)
    row8 = lax.broadcasted_iota(jnp.int32, (8, 4 * K), 0)
    lane8 = lane_of((8, 4 * K)) < 2 * K
    is_sol = lax.rem(row8, 4) < 2
    sign = jnp.where(is_sol, jnp.where(lane8, 1.0, 0.0), jnp.where(lane8, 0.0, -1.0))

    gathered_patch(pc, PC)
    total = jnp.sum(pc[...], axis=0)
    moved = [total] + [pltpu.roll(total, 128 - K * i, 1) for i in range(1, 8)]
    a2 = eliminate(jnp.concatenate(moved, axis=0)[:, :K], rows8)
    a2 = jnp.concatenate((a2, a2, a2, a2), axis=1)
    chi = a2.astype(BF16).astype(F32)
    coeffs = (jnp.where(row8 < 4, chi, a2 - chi) * sign).astype(BF16)
    for p in range(PD):
        t = dot(coeffs, jnp.concatenate((d2h[PD + p], d2w[PD + p], imh[p], iml[p]), axis=0), NN)
        both_o[p] += t[:4] + t[4:]

    for ref, kind in ((mg, M), (pg, PA), (wg, WA), (pc, PC)):
        handle(ref.at[pl.ds(0, np_ - 1)], kind).wait_send()
    for ref, kind in ((lg, L), (gh, ZH), (gl, ZL)):
        handle(ref.at[pl.ds(0, nz - 1)], kind).wait_send()
    for ref, kind in ((hlh, HL), (hrh, HR)):
        handle(ref, kind).wait_send()
    for ref, kind in ((sl, OL), (sl, OR), (wh, WL), (wh, WR), (wl, WLL), (wl, WRL)):
        handle(ref.at[mid], kind).wait_send()


def on_device(*args):
    args = list(args)
    args[2] = args[2].T
    args[8] = jnp.swapaxes(args[8], 1, 2)
    args = [pltpu.with_memory_space_constraint(x, pltpu.HBM) for x in args]
    np_, nz = lax.axis_size("patch"), lax.axis_size("rhs")
    vm = pltpu.VMEM
    sem = pltpu.SemaphoreType.DMA
    chunks = vm((nz, PD, 2, W), BF16)
    three = vm((3 * PD, K, W), BF16)
    one = vm((PD, K, W), BF16)
    message = vm((np_, 8, 128), F32)
    scratch = [
        vm((PD, 2, W), F32),
        vm((PD, NB, W, W), BF16),
        pltpu.SMEM((NB, PD), jnp.int32),
        vm((PD, E, W), F32),
        vm((PD, E, E), F32),
        pltpu.SMEM((1, FL), jnp.int32),
        vm((1, FL, E, E), F32),
        vm((PD, E, E), F32),
        vm((PD, E, W), F32),
        chunks, chunks, chunks, chunks,
        three, three, three, three, three, three, one, one,
        vm((PD, K, W), F32),
        vm((2 * E, PD * W), BF16),
        vm((2 * E, FL * E), BF16),
        vm((PD, 2 * E, W), BF16),
        vm((np_, 2, 128), F32),
        vm((nz, 2, 128), F32),
        vm((K, 128), F32),
        message, message,
        vm((np_, 2, 128), F32),
        vm((3 * K, 128), F32),
        sem((9,)), sem((nz,)), sem((15,)), sem((15,)),
    ]
    out = pl.pallas_call(
        kernel,
        out_shape=pltpu.VMEM((PD, 4, W), F32),
        in_specs=[pl.BlockSpec(memory_space=pltpu.MemorySpace.HBM)] * 9,
        out_specs=pl.BlockSpec(memory_space=pltpu.VMEM),
        scratch_shapes=scratch,
        compiler_params=pltpu.CompilerParams(
            collective_id=0, has_side_effects=True, vmem_limit_bytes=60_000_000
        ),
    )(*args)
    return out[:, :2], out[:, 2:]


def solution(mesh):
    return jax.shard_map(
        on_device,
        mesh=mesh,
        in_specs=(
            P("patch", "rhs", None),
            P("patch", None, None, None),
            P("patch", None),
            P("patch", None, None),
            P("patch", None, None),
            P("patch", None),
            P("patch", None, None, None),
            P("patch", None, None),
            P("patch", None, None),
        ),
        out_specs=(P("patch", "rhs", None), P("patch", "rhs", None)),
        check_vma=False,
    )
```

```python
import jax
import jax.numpy as jnp
from jax import lax
from jax.experimental import pallas as pl
from jax.experimental.pallas import tpu as pltpu
from jax.sharding import PartitionSpec as P

F32 = jnp.float32
BF16 = jnp.bfloat16
HIGH = lax.Precision.HIGHEST
MESH = pl.DeviceIdType.MESH
PD, K, W, E, NB, FL = 8, 16, 384, 64, 4, 4
NT = (((1,), (1,)), ((), ()))
NN = (((1,), (0,)), ((), ()))


def dot(a, b, dims=NT, precision=None):
    return lax.dot_general(a, b, dims, precision=precision, preferred_element_type=F32)


def split(x):
    hi = x.astype(BF16)
    return hi, (x - hi.astype(F32)).astype(BF16)


def folded(x):
    return x + pltpu.roll(x, 64, 1)


def lane_of(shape):
    return lax.broadcasted_iota(jnp.int32, shape, 1)


def eliminate(top, *others):
    a = jnp.concatenate((top, *others), axis=0)
    lanes = lane_of(a.shape)
    group = 8
    for base in range(0, K, group):
        columns = [jnp.broadcast_to(a[:, k : k + 1], a.shape) for k in range(base, base + group)]
        for i in range(group):
            k = base + i
            column = columns[i]
            inverse = 1.0 / column[k : k + 1, :]
            scaled = column * inverse
            for j in range(i + 1, group):
                columns[j] = columns[j] - scaled * columns[j][k : k + 1, :]
            a = jnp.where(lanes == k, scaled, a - scaled * a[k : k + 1, :])
    return a[K:]


def packed_grams(rows, high, low):
    full = dot(rows, high) + dot(rows, low)
    a = full[:K] + full[K : 2 * K]
    b = full[2 * K : 3 * K] + full[3 * K :]
    return jnp.concatenate((a[:8], a[8:], b[:8], b[8:]), axis=1)


def unpacked_grams(total):
    def at(lane):
        return pltpu.roll(total, 128 - lane, 1) if lane else total

    def block(lane):
        return jnp.concatenate((at(lane), at(lane + 2 * K)), axis=0)[:, :K]

    return block(0), block(K), block(4 * K), block(5 * K)


def far_first():
    order = [(dy, dx, dc) for dy in range(4) for dx in range(4) for dc in range(2)]
    order.remove((0, 0, 0))
    return sorted(order, key=lambda t: -(min(t[0], 4 - t[0]) + min(t[1], 4 - t[1])))


def product_split(left, right):
    rhi, rlo = split(right)
    twice = jnp.concatenate((left, left), axis=1)
    hi = twice.astype(BF16)
    lo = (twice - hi.astype(F32)).astype(BF16)
    t = dot(jnp.concatenate((hi, lo), axis=0), jnp.concatenate((rhi, rlo), axis=0), NN)
    return split(t[:E] + t[E:])


def kernel(
    rhs_h, near_h, nbr_h, up_h, su_h, fl_h, tr_h, sd_h, dn_h,
    both_o,
    rhs_v, near_v, nbr_s, up_v, su_v, fl_s, tr_v, sd_v, dn_v,
    gh, gl, hlh, hrh, sh, sl, wh, wl, d2h, d2w, imh, iml, nf,
    cst, tst, dst, mg, lg, lf, pg, wg, pc, cf,
    local_sem, z_recv, sends, recvs,
):
    me = lax.axis_index("patch")
    z = lax.axis_index("rhs")
    np_, nz = lax.axis_size("patch"), lax.axis_size("rhs")
    left, right = lax.rem(me + np_ - 1, np_), lax.rem(me + 1, np_)
    core, chip = lax.rem(me, 2), me // 2
    cx, cy = lax.rem(chip, 4), chip // 4
    peers = [
        (lax.rem(cy + dy, 4) * 4 + lax.rem(cx + dx, 4)) * 2 + lax.rem(core + dc, 2)
        for dy, dx, dc in far_first()
    ]
    z_order = (4, 3, 5, 2, 6, 1, 7)
    z_peers = [lax.rem(z + d, nz) for d in z_order]

    def load(i, src, dst):
        copy = pltpu.make_async_copy(src, dst, local_sem.at[i])
        copy.start()
        return copy

    c_rhs = load(0, rhs_h, rhs_v)
    barrier = pltpu.get_barrier_semaphore()
    for to in z_peers:
        pl.semaphore_signal(barrier, inc=1, device_id=(me, to), device_id_type=MESH)
    for to in peers:
        pl.semaphore_signal(barrier, inc=1, device_id=(to, z), device_id_type=MESH)
    c_up = load(1, up_h, up_v)
    c_su = load(2, su_h, su_v)
    c_tr = load(5, tr_h, tr_v)
    c_sd = load(6, sd_h, sd_v)
    c_dn = load(7, dn_h, dn_v)
    c_fl = load(4, fl_h, fl_s)
    c_nbr = load(3, nbr_h, nbr_s)
    M, L, PA, WA, PC, ZH, ZL, HL, HR, OL, OR, WL, WR, WLL, WRL = range(15)

    def send(src, dst, kind, device, recv=None):
        pltpu.make_async_remote_copy(
            src_ref=src,
            dst_ref=dst,
            send_sem=sends.at[kind],
            recv_sem=recvs.at[kind] if recv is None else recv,
            device_id=device,
            device_id_type=MESH,
        ).start()

    def handle(ref, kind, recv=None):
        return pltpu.make_async_remote_copy(
            src_ref=ref,
            dst_ref=ref,
            send_sem=sends.at[kind],
            recv_sem=recvs.at[kind] if recv is None else recv,
            device_id=(right, z),
            device_id_type=MESH,
        )

    def spread_patch(buf, kind):
        for to in peers:
            send(buf.at[me], buf.at[me], kind, (to, z))

    def gathered_patch(buf, kind):
        handle(buf.at[pl.ds(0, np_ - 1)], kind).wait_recv()

    def spread_z(buf, kind, recv=None):
        for to in z_peers:
            send(buf.at[z], buf.at[z], kind, (me, to), recv)

    def forward(zz):
        send(gh.at[zz], hlh.at[zz], HL, (right, z))
        send(gh.at[zz], hrh.at[zz], HR, (left, z))

    c_rhs.wait()
    own_hi, own_lo = [], []
    for p in range(PD):
        hi, lo = split(rhs_v[p])
        gh[z, p] = hi
        gl[z, p] = lo
        own_hi.append(hi)
        own_lo.append(lo)
    own_hi = jnp.concatenate(own_hi, axis=1)
    own_lo = jnp.concatenate(own_lo, axis=1)

    pl.semaphore_wait(barrier, np_ + nz - 2)
    spread_z(gh, ZH, z_recv.at[z])
    forward(z)

    c_up.wait()
    c_su.wait()
    c_near = load(8, near_h, near_v)
    for p in range(PD):
        hi, lo = product_split(su_v[p], up_v[p])
        cst[:E, p * W : (p + 1) * W] = hi
        cst[E:, p * W : (p + 1) * W] = lo
    mg[me] = folded(dot(own_hi, cst[...]) + dot(own_lo, cst[...]))
    spread_patch(mg, M)

    def take(d):
        zz = lax.rem(z + d, nz)
        handle(gh.at[zz], ZH, z_recv.at[zz]).wait_recv()
        forward(zz)

    c_tr.wait()
    for i in range(2):
        hi, lo = split(jnp.concatenate((tr_v[0, 2 * i], tr_v[0, 2 * i + 1]), axis=1))
        tst[:E, i * 128 : (i + 1) * 128] = hi
        tst[E:, i * 128 : (i + 1) * 128] = lo

    for d in (1, 7, 2, 6, 3, 5, 4):
        take(d)

    def assembled(buf, dest, base):
        for zz in range(8):
            for p in range(PD):
                dest[base + p, 2 * zz : 2 * zz + 2, :] = buf[zz, p]

    c_fl.wait()
    src = [fl_s[0, j] for j in range(FL)]
    spread_z(gl, ZL)
    gathered_patch(mg, M)
    low2 = lane_of((2, 128)) < E
    chosen = jnp.concatenate(
        (jnp.where(low2, mg[src[0]], mg[src[1]]), jnp.where(low2, mg[src[2]], mg[src[3]])), axis=1
    )
    hi, lo = split(chosen)
    lg[z] = folded(dot(hi, tst[...]) + dot(lo, tst[...]))
    spread_z(lg, L)

    assembled(gh, sh, PD)
    c_sd.wait()
    c_dn.wait()
    for p in range(PD):
        hi, lo = product_split(sd_v[p].T, dn_v[p])
        dst[p, :E] = hi
        dst[p, E:] = lo

    c_near.wait()
    for p in range(PD):
        nf[p] = dot(near_v[p, 0], sh[PD + p]).T

    handle(hlh, HL).wait_recv()
    assembled(hlh, sh, 0)
    handle(hrh, HR).wait_recv()
    assembled(hrh, sh, 2 * PD)

    c_nbr.wait()
    first = me * PD - PD
    total_patches = np_ * PD
    ids = [
        [
            jnp.minimum(lax.rem(nbr_s[j, p] - first + 2 * total_patches, total_patches), 3 * PD - 1)
            for j in range(NB)
        ]
        for p in range(PD)
    ]

    def near_of(p, field, start):
        blocks = jnp.concatenate([near_v[p, j] for j in range(start, NB)], axis=1)
        picked = jnp.concatenate([field[ids[p][j]] for j in range(start, NB)], axis=1)
        return dot(blocks, picked).T if p % 4 != 3 else dot(picked, blocks)

    def far_of(p, lcat):
        far = dot(lcat, dst[p], NN)
        return far[:K] + far[K:]

    for p in range(PD):
        nf[p] += near_of(p, sh, 1)

    handle(gl.at[pl.ds(0, nz - 1)], ZL).wait_recv()
    assembled(gl, sl, PD)
    mid = pl.ds(PD, PD)
    send(sl.at[mid], sl.at[pl.ds(0, PD)], OL, (right, z))
    send(sl.at[mid], sl.at[pl.ds(2 * PD, PD)], OR, (left, z))

    handle(lg.at[pl.ds(0, nz - 1)], L).wait_recv()
    for zz in range(8):
        lf[2 * zz : 2 * zz + 2, :] = lg[zz]
    local0 = lf[...]
    lcat = jnp.concatenate(split(local0), axis=0)
    for p in range(PD):
        hi, lo = split(nf[p] + far_of(p, lcat))
        wh[PD + p] = hi
        wl[PD + p] = lo

    def joined(base, *refs):
        return jnp.concatenate(
            [jnp.concatenate([ref[base + p] for p in range(PD)], axis=1) for ref in refs], axis=0
        )

    pg[me] = packed_grams(joined(PD, sh, sl, wh, wl), joined(PD, wh, sh), joined(PD, wl, sl))
    spread_patch(pg, PA)
    up_w = dot(joined(PD, wh, wl), cst[...])
    up_w = folded(up_w[:K] + up_w[K:])
    low8 = lane_of((8, 128)) < E
    wg[me] = jnp.where(low8, up_w[:8], up_w[8:])
    spread_patch(wg, WA)
    send(wh.at[mid], wh.at[pl.ds(0, PD)], WL, (right, z))
    send(wh.at[mid], wh.at[pl.ds(2 * PD, PD)], WR, (left, z))
    send(wl.at[mid], wl.at[pl.ds(0, PD)], WLL, (right, z))
    send(wl.at[mid], wl.at[pl.ds(2 * PD, PD)], WRL, (left, z))

    gathered_patch(pg, PA)
    gg, rr, qq, gt = unpacked_grams(jnp.sum(pg[...], axis=0))
    eye = (lax.broadcasted_iota(jnp.int32, (K, K), 0) == lane_of((K, K))).astype(F32)
    a1 = eliminate(0.5 * (gg + gt), rr)
    inv = eliminate(rr, eye)
    blank = jnp.zeros((2 * K, K), F32)
    aq = dot(a1, qq, NN, HIGH) - gg
    ag = dot(a1, gg, NT, HIGH)
    ka = dot(inv, a1, NN, HIGH)
    row16, lane64 = lax.broadcasted_iota(jnp.int32, (K, 4 * K), 0), lane_of((K, 4 * K))
    twice = jnp.where((lane64 == row16) | (lane64 == row16 + K), 2.0, 0.0)
    minus = jnp.concatenate((jnp.zeros((K, 2 * K), F32), -a1, -a1), axis=1)
    first = dot(aq, jnp.concatenate((ka, ka, blank), axis=0), NT, HIGH)
    first = first - dot(ag, jnp.concatenate((inv, inv, blank), axis=0), NT, HIGH) + twice
    mixer = first + minus
    first_co, second_co = first[:, :K], -a1
    rr1 = rr - ag + dot(aq, a1, NT, HIGH)
    mhi = mixer.astype(BF16).astype(F32)
    mixer = jnp.concatenate((mhi, mixer - mhi), axis=0).astype(BF16)

    def mixed(i):
        t = dot(mixer, jnp.concatenate((sh[i], sl[i], wh[i], wl[i]), axis=0), NN)
        hi, lo = split(t[:K] + t[K:])
        d2h[i] = hi
        if PD <= i < 2 * PD:
            d2w[i] = lo

    for i in range(PD, 2 * PD):
        mixed(i)
    for p in range(PD):
        nf[p] = dot(near_v[p, 0], d2h[PD + p]).T

    for base, kinds in ((0, (OL, WL, WLL)), (2 * PD, (OR, WR, WRL))):
        for kind, ref in zip(kinds, (sl, wh, wl)):
            handle(ref.at[pl.ds(base, PD)], kind).wait_recv()
        for i in range(base, base + PD):
            mixed(i)

    gathered_patch(wg, WA)
    us = [wg[src[j]] for j in range(FL)]
    rs = [pltpu.roll(u, E, 1) for u in us]
    chosen = jnp.concatenate(
        (
            jnp.concatenate((jnp.where(low8, us[0], rs[1]), jnp.where(low8, rs[0], us[1])), axis=0),
            jnp.concatenate((jnp.where(low8, us[2], rs[3]), jnp.where(low8, rs[2], us[3])), axis=0),
        ),
        axis=1,
    )
    hi, lo = split(chosen)
    local_w = folded(dot(hi, tst[...]) + dot(lo, tst[...]))
    local2 = dot(first_co, local0, NN, HIGH) + dot(second_co, local_w, NN, HIGH)
    lcat = jnp.concatenate(split(local2), axis=0)

    for p in range(PD):
        hi, lo = split(nf[p] + near_of(p, d2h, 1) + far_of(p, lcat))
        imh[p] = hi
        iml[p] = lo

    def crossed(base_a, ah, al, base_b, bh, bl):
        rows = jnp.concatenate((joined(base_a, ah), joined(base_a, al)), axis=0)
        t = dot(rows, joined(base_b, bh)) + dot(rows, joined(base_b, bl))
        return t[:K] + t[K:]

    half = crossed(PD, d2h, d2w, 0, imh, iml) + crossed(0, imh, iml, PD, d2h, d2w)
    half = 0.5 * half
    pc[me] = jnp.concatenate([half[2 * i : 2 * i + 2] for i in range(8)], axis=1)
    spread_patch(pc, PC)

    cf[0:K, 0:K] = a1
    cf[K : 2 * K, 0:K] = rr1
    mine_a1, mine_rr1 = cf[pl.ds(2 * z, 2), 0:K], cf[pl.ds(K + 2 * z, 2), 0:K]
    cf[2 * K : 3 * K, 0:K] = eye
    mine_eye = cf[pl.ds(2 * K + 2 * z, 2), 0:K]
    none = jnp.zeros((2, K), F32)
    coeffs = jnp.concatenate(
        (
            jnp.concatenate((mine_a1, mine_a1, none, none), axis=1),
            jnp.concatenate((mine_eye, mine_eye, -mine_a1, -mine_a1), axis=1),
        ),
        axis=0,
    )
    chi = coeffs.astype(BF16).astype(F32)
    coeffs = jnp.concatenate((chi, coeffs - chi), axis=0).astype(BF16)
    for p in range(PD):
        q = PD + p
        t = dot(coeffs, jnp.concatenate((sh[q], sl[q], wh[q], wl[q]), axis=0), NN)
        both_o[p] = t[:4] + t[4:]
    rows8 = jnp.concatenate((mine_rr1,) * 4, axis=0)
    row8 = lax.broadcasted_iota(jnp.int32, (8, 4 * K), 0)
    lane8 = lane_of((8, 4 * K)) < 2 * K
    is_sol = lax.rem(row8, 4) < 2
    sign = jnp.where(is_sol, jnp.where(lane8, 1.0, 0.0), jnp.where(lane8, 0.0, -1.0))

    gathered_patch(pc, PC)
    total = jnp.sum(pc[...], axis=0)
    moved = [total] + [pltpu.roll(total, 128 - K * i, 1) for i in range(1, 8)]
    a2 = eliminate(jnp.concatenate(moved, axis=0)[:, :K], rows8)
    a2 = jnp.concatenate((a2, a2, a2, a2), axis=1)
    chi = a2.astype(BF16).astype(F32)
    coeffs = (jnp.where(row8 < 4, chi, a2 - chi) * sign).astype(BF16)
    for p in range(PD):
        t = dot(coeffs, jnp.concatenate((d2h[PD + p], d2w[PD + p], imh[p], iml[p]), axis=0), NN)
        both_o[p] += t[:4] + t[4:]

    for ref, kind in ((mg, M), (pg, PA), (wg, WA), (pc, PC)):
        handle(ref.at[pl.ds(0, np_ - 1)], kind).wait_send()
    for ref, kind in ((lg, L), (gh, ZH), (gl, ZL)):
        handle(ref.at[pl.ds(0, nz - 1)], kind).wait_send()
    for ref, kind in ((hlh, HL), (hrh, HR)):
        handle(ref, kind).wait_send()
    for ref, kind in ((sl, OL), (sl, OR), (wh, WL), (wh, WR), (wl, WLL), (wl, WRL)):
        handle(ref.at[mid], kind).wait_send()


def on_device(*args):
    args = list(args)
    args[2] = args[2].T
    args[8] = jnp.swapaxes(args[8], 1, 2)
    args = [pltpu.with_memory_space_constraint(x, pltpu.HBM) for x in args]
    np_, nz = lax.axis_size("patch"), lax.axis_size("rhs")
    vm = pltpu.VMEM
    sem = pltpu.SemaphoreType.DMA
    chunks = vm((nz, PD, 2, W), BF16)
    three = vm((3 * PD, K, W), BF16)
    one = vm((PD, K, W), BF16)
    message = vm((np_, 8, 128), F32)
    scratch = [
        vm((PD, 2, W), F32),
        vm((PD, NB, W, W), BF16),
        pltpu.SMEM((NB, PD), jnp.int32),
        vm((PD, E, W), F32),
        vm((PD, E, E), F32),
        pltpu.SMEM((1, FL), jnp.int32),
        vm((1, FL, E, E), F32),
        vm((PD, E, E), F32),
        vm((PD, E, W), F32),
        chunks, chunks, chunks, chunks,
        three, three, three, three, three, three, one, one,
        vm((PD, K, W), F32),
        vm((2 * E, PD * W), BF16),
        vm((2 * E, FL * E), BF16),
        vm((PD, 2 * E, W), BF16),
        vm((np_, 2, 128), F32),
        vm((nz, 2, 128), F32),
        vm((K, 128), F32),
        message, message,
        vm((np_, 2, 128), F32),
        vm((3 * K, 128), F32),
        sem((9,)), sem((nz,)), sem((15,)), sem((15,)),
    ]
    out = pl.pallas_call(
        kernel,
        out_shape=pltpu.VMEM((PD, 4, W), F32),
        in_specs=[pl.BlockSpec(memory_space=pltpu.MemorySpace.HBM)] * 9,
        out_specs=pl.BlockSpec(memory_space=pltpu.VMEM),
        scratch_shapes=scratch,
        compiler_params=pltpu.CompilerParams(
            collective_id=0, has_side_effects=True, vmem_limit_bytes=60_000_000
        ),
    )(*args)
    return out[:, :2], out[:, 2:]


def solution(mesh):
    return jax.shard_map(
        on_device,
        mesh=mesh,
        in_specs=(
            P("patch", "rhs", None),
            P("patch", None, None, None),
            P("patch", None),
            P("patch", None, None),
            P("patch", None, None),
            P("patch", None),
            P("patch", None, None, None),
            P("patch", None, None),
            P("patch", None, None),
        ),
        out_specs=(P("patch", "rhs", None), P("patch", "rhs", None)),
        check_vma=False,
    )
```
